32 devices in a mesh: prow: 4 (over x, core), pcol: 8 (over z, y).
Axes of the slice: x: 2, y: 2, z: 4, core: 2. Of those that a mesh axis runs over, the one named last changes fastest.
Arguments:
- slab: float32 [16384, 2048], P('prow', 'pcol'), may hold values from -6 to 6
- panel: float32 [16384, 512], P(('prow', 'pcol')), may hold values from -0.25 to 0.25
- pivots: int32 [512], replicated, may hold values from 0 to 16383, as said below
- inv_lower: float32 [512, 512], replicated, as said below
- inv_upper: float32 [512, 512], replicated, as said below
Outputs:
- updated: float32 [16384, 2048], P('prow', 'pcol')
The draws below stay inside these ranges and needn't reach their ends.
Inputs may be any that keep to these rules, and one draw needn't show every extreme that they name: `pivots`: 512 distinct row indices. `inv_lower`: unit lower triangular. `inv_upper`: upper triangular with a positive diagonal.
All inputs are finite; a program needn't handle non-finite values.
Results may differ from the reference program's by a relative error of at most 0.000061.
Values sent between devices are 32-bit elements; how exact they have to be, the bound alone decides.
A program may use at most 64 MiB of HBM per device.

```python
import jax
import jax.numpy as jnp
from jax import lax

NB = 512
ROWS_DEV = 4096
NS_DEV = 256
M = 16384
NS = 2048
N_PROW = 4
N_PCOL = 8


def draw_pivots(key, part):
    order = jax.random.permutation(jax.random.fold_in(key, 11), ROWS_DEV * N_PROW)
    return order[:NB].astype(jnp.int32)


def draw_inv_lower(key, part):
    sub_key = jax.random.fold_in(key, 23)
    entries = jax.random.normal(sub_key, (NB, NB), jnp.float32)
    return jnp.tril(entries, -1) * NB ** (-0.5) + jnp.eye(NB, dtype=jnp.float32)


def draw_inv_upper(key, part):
    sub_key = jax.random.fold_in(key, 37)
    diag_key = jax.random.fold_in(key, 41)
    entries = jax.random.normal(sub_key, (NB, NB), jnp.float32)
    diagonal = jax.random.uniform(diag_key, (NB,), jnp.float32, 0.5, 1.5)
    return jnp.triu(entries, 1) * NB ** (-0.5) + jnp.diag(diagonal)


def shard_levels(key, extent, split, least, high):
    def one(dim, parts):
        steps = jax.random.uniform(jax.random.fold_in(jax.random.fold_in(key, 6), dim), (parts,), jnp.float32, least / len(split), high / len(split))
        return jnp.repeat(jnp.exp(steps), extent[dim] // parts).reshape((-1,) + (1,) * (len(extent) - dim - 1))

    gain = one(*split[0])
    for cut in split[1:]:
        gain = gain * one(*cut)
    return gain


def normal_values(rng, shape, scale, bound, split=(), kind=jnp.bfloat16):
    values = scale * jax.random.normal(rng, shape, jnp.float32)
    if split:
        values = values * shard_levels(rng, shape, split, -0.22, 0.18)
    return jnp.clip(values, -bound, bound).astype(kind)


def setup_inputs(seed: int = 0) -> dict:
    arg_keys = jax.random.split(jax.random.key(seed), 6)
    return {
        "slab": normal_values(arg_keys[0], (M, NS), 1.0, 6.0, ((0, 4), (1, 8)), jnp.float32),
        "panel": normal_values(arg_keys[1], (M, NB), NB ** -0.5, 0.25, ((0, 32),), jnp.float32),
        "pivots": draw_pivots(jax.random.fold_in(arg_keys[5], 71), 0),
        "inv_lower": draw_inv_lower(jax.random.fold_in(arg_keys[5], 71), 0),
        "inv_upper": draw_inv_upper(jax.random.fold_in(arg_keys[5], 71), 0),
    }


def reference(slab, panel, pivots, inv_lower, inv_upper):
    pivot_rows = jnp.take(slab, pivots.astype(jnp.int32), axis=0)
    upper_block = jnp.dot(inv_lower, pivot_rows, precision=lax.Precision.HIGHEST, preferred_element_type=jnp.float32)
    panel_blocks = panel.reshape(N_PROW, ROWS_DEV, NB)
    slab_blocks = slab.reshape(N_PROW, ROWS_DEV, NS_DEV * N_PCOL)

    def one_block(operands):
        panel_block, slab_block = operands
        lower_rows = jnp.dot(panel_block, inv_upper, precision=lax.Precision.HIGHEST, preferred_element_type=jnp.float32)
        product = jnp.dot(lower_rows, upper_block, precision=lax.Precision.HIGHEST, preferred_element_type=jnp.float32)
        return slab_block - product

    updated = lax.map(one_block, (panel_blocks, slab_blocks)).reshape(slab.shape)
    updated = updated.at[pivots.astype(jnp.int32)].set(upper_block)
    return updated
```

```python
import functools

import jax
import jax.numpy as jnp
from jax import lax
from jax.experimental import pallas as pl
from jax.experimental.pallas import tpu as pltpu
from jax.sharding import PartitionSpec as P

MESH = pl.DeviceIdType.MESH
HIGHEST = lax.Precision.HIGHEST
F32 = jnp.float32
BF16 = jnp.bfloat16


def dot(a, b):
    return jnp.dot(a, b, precision=HIGHEST, preferred_element_type=F32)


def split(a):
    high = a.astype(BF16)
    return high, (a - high.astype(F32)).astype(BF16)


def dot_split(a_high, a_low, b_high, b_low):
    rows = a_high.shape[0]
    both = jnp.dot(
        jnp.concatenate([a_high, a_low], axis=0), b_high, preferred_element_type=F32
    )
    cross = jnp.dot(a_high, b_low, preferred_element_type=F32)
    return both[:rows] + (both[rows:] + cross)


def kernel(
    n_x, n_z, parts, chunks, early,
    slab_ref, panel_ref, pivots_ref, pivot_row_ref, inv_lower_ref, inv_upper_ref,
    out_ref,
    raw, raw_peer, lower, lower_own, stage, landed, inv_lower, inv_upper, inv_split,
    picked, partner_part, chip_sum, from_x, total, halves, upper,
    load_sem, link_send, link_recv, product_send, product_recv,
    pick_send, pick_recv, x_send, x_recv, half_send, half_recv, peer_send, peer_recv,
):
    slab = out_ref
    prow = lax.axis_index("prow")
    pcol = lax.axis_index("pcol")
    x, core = prow // 2, prow % 2
    z, y = pcol // 2, pcol % 2
    rows, nb = panel_ref.shape
    piece, chunk = rows // parts, rows // chunks
    row_count, columns = slab_ref.shape
    half = columns // 2
    first_row = prow * row_count
    hops = parts * (n_z - 1) // 2
    partner = {"prow": x * 2 + 1 - core}
    peer = {"pcol": z * 2 + 1 - y}
    right = {"pcol": lax.rem(z + 1, n_z) * 2 + y}
    left = {"pcol": lax.rem(z + n_z - 1, n_z) * 2 + y}
    others = [{"prow": lax.rem(x + o, n_x) * 2 + core} for o in range(1, n_x)]

    panel_load = pltpu.make_async_copy(panel_ref, raw.at[z], load_sem.at[0])
    slab_load = pltpu.make_async_copy(slab_ref, slab, load_sem.at[1])
    upper_load = pltpu.make_async_copy(inv_upper_ref, inv_upper, load_sem.at[2])
    lower_load = pltpu.make_async_copy(inv_lower_ref, inv_lower, load_sem.at[3])
    panel_load.start()

    barrier = pltpu.get_barrier_semaphore()
    neighbours = [partner, peer, right, left] + others
    for device in neighbours:
        pl.semaphore_signal(barrier, inc=1, device_id=device, device_id_type=MESH)
    slab_load.start()
    upper_load.start()
    lower_load.start()
    pl.semaphore_wait(barrier, len(neighbours))

    def remote(source, target, send_sem, recv_sem, device):
        return pltpu.make_async_remote_copy(
            src_ref=source, dst_ref=target, send_sem=send_sem, recv_sem=recv_sem,
            device_id=device, device_id_type=MESH,
        )

    def place(direction, q, away):
        distance = q // parts + away
        turn = n_z - distance if direction == 0 else distance
        block = lax.rem(z + turn, n_z)
        part = q % parts if direction == 0 else parts - 1 - q % parts
        return block, part * piece

    def link(direction, q, away):
        block, start = place(direction, q, away)
        spot = raw.at[block, pl.ds(pl.multiple_of(start, 8), piece)]
        index = direction * hops + q
        return remote(
            spot, spot, link_send.at[index], link_recv.at[index],
            right if direction == 0 else left,
        )

    def peer_copy(g):
        span = pl.ds(g * chunk, chunk)
        return remote(
            raw.at[z, span], raw_peer.at[span], peer_send.at[g], peer_recv.at[g], peer
        )

    panel_load.wait()
    for q in range(min(parts, hops)):
        for direction in (0, 1):
            link(direction, q, 0).start()
    for g in range(chunks - 1):
        peer_copy(g).start()

    slab_load.wait()

    def pick(k, carry):
        local = pivots_ref[k] - first_row
        inside = (local >= 0) & (local < row_count)
        row = slab[pl.ds(jnp.where(inside, local, 0), 1), :]
        row = jnp.where(inside, row, 0.0)
        picked[0, pl.ds(k, 1), :] = row[:, :half]
        picked[1, pl.ds(k, 1), :] = row[:, half:]
        return carry

    lax.fori_loop(0, nb, pick, 0, unroll=8)

    pick_copy = remote(picked.at[1 - core], partner_part, pick_send, pick_recv, partner)
    pick_copy.start()
    upper_load.wait()
    lower_load.wait()
    inv_split[0], inv_split[1] = split(inv_upper[...])
    pick_copy.wait()
    chip_sum[...] = picked[core] + partner_part[...]
    x_copies = [
        remote(chip_sum, from_x.at[i], x_send.at[i], x_recv.at[i], device)
        for i, device in enumerate(others)
    ]
    for copy in x_copies:
        copy.start()

    def pivot_hits(start, count):
        ids = first_row + start + lax.broadcasted_iota(jnp.int32, (count, nb), 0)
        return jnp.where(ids == pivot_row_ref[...], 1.0, 0.0)

    def is_pivot(hits):
        return jnp.max(hits, axis=1, keepdims=True) > 0.0

    def solve(rows_in, hits):
        high, low = split(rows_in)
        solved = dot_split(high, low, inv_split[0], inv_split[1])
        return split(jnp.where(is_pivot(hits), -hits, solved))

    def clear(i, carry):
        start = pl.multiple_of(i * chunk, 8)
        span = pl.ds(start, chunk)
        slab[span, :] = jnp.where(
            is_pivot(pivot_hits(start, chunk)), 0.0, slab[span, :]
        )
        return carry

    lax.fori_loop(0, row_count // chunk, clear, 0)

    def solve_own(g, carry):
        span = pl.ds(pl.multiple_of(g * chunk, 8), chunk)
        hits = pivot_hits((z * 2 + y) * rows + g * chunk, chunk)
        lower_own[0, span, :], lower_own[1, span, :] = solve(raw[z, span, :], hits)
        return carry

    lax.fori_loop(0, chunks, solve_own, 0)

    def prepare(q):
        rows_in, hits = [], []
        for direction in (0, 1):
            link(direction, q, 1).wait_recv()

            @pl.when(q + parts < hops)
            def _():
                link(direction, q + parts, 0).start()

            block, start = place(direction, q, 1)
            rows_in.append(raw[block, pl.ds(pl.multiple_of(start, 8), piece), :])
            hits.append(pivot_hits((block * 2 + y) * rows + start, piece))
        lower[0, q], lower[1, q] = solve(
            jnp.concatenate(rows_in, axis=0), jnp.concatenate(hits, axis=0)
        )

    first, second = min(early[0], hops), min(early[1], hops)
    lax.fori_loop(0, first, lambda q, c: (prepare(q), c)[1], 0)

    for copy in x_copies:
        copy.wait()
    summed = chip_sum[...]
    for o in range(1, n_x):
        summed = summed + from_x[o - 1]
    total[...] = summed
    halves[core] = dot(inv_lower[...], total[...])
    to_peer = remote(
        halves.at[core], halves.at[2 + core], half_send.at[0], half_recv.at[0], peer
    )
    to_partner = remote(
        halves.at[core], halves.at[core], half_send.at[1], half_recv.at[1], partner
    )
    to_peer.start()
    to_partner.start()
    peer_copy(chunks - 1).start()

    lax.fori_loop(first, second, lambda q, c: (prepare(q), c)[1], 0)

    to_peer.wait()
    onward = remote(
        halves.at[2 + core], halves.at[2 + core], half_send.at[2], half_recv.at[2], partner
    )
    onward.start()
    to_partner.wait()

    def split_upper(i):
        span = slice(i * half, (i + 1) * half)
        upper[0, :, span], upper[1, :, span] = split(halves[i])

    split_upper(0)
    split_upper(1)
    onward.wait()
    split_upper(2)
    split_upper(3)

    def product_copy(q):
        return remote(
            stage.at[q], landed.at[q], product_send.at[q], product_recv.at[q], peer
        )

    def subtract(start, count, product):
        span = pl.ds(pl.multiple_of(start, 8), count)
        slab[span, :] = slab[span, :] - product

    def subtract_both(q, side, product):
        for direction in (0, 1):
            block, start = place(direction, q, 1)
            subtract(
                (block * 2 + side) * rows + start, piece,
                product[direction * piece:(direction + 1) * piece],
            )

    def multiply(q):
        products = dot_split(lower[0, q], lower[1, q], upper[0], upper[1])
        stage[q] = products[:, columns:]
        product_copy(q).start()
        subtract_both(q, y, products[:, :columns])

    def take(q, carry):
        product_copy(q).wait_recv()
        subtract_both(q, 1 - y, landed[q])
        return carry

    def multiply_own(g):
        span = pl.ds(pl.multiple_of(g * chunk, 8), chunk)
        product = dot_split(
            lower_own[0, span, :], lower_own[1, span, :],
            upper[0, :, :columns], upper[1, :, :columns],
        )
        subtract((z * 2 + y) * rows + g * chunk, chunk, product)

    def multiply_peer(g):
        peer_copy(g).wait_recv()
        span = pl.ds(pl.multiple_of(g * chunk, 8), chunk)
        start = (z * 2 + 1 - y) * rows + g * chunk
        high, low = solve(raw_peer[span, :], pivot_hits(start, chunk))
        product = dot_split(high, low, upper[0, :, :columns], upper[1, :, :columns])
        subtract(start, chunk, product)

    lax.fori_loop(0, second, lambda q, c: (multiply(q), c)[1], 0)

    def taken(i):
        return jnp.minimum(2 * i, jnp.maximum(second + i - 1, 0))

    def steady(i, carry):
        q = second + i
        prepare(q)
        multiply(q)

        @pl.when(i < chunks)
        def _():
            multiply_own(i)
            multiply_peer(i)

        lax.fori_loop(taken(i), taken(i + 1), take, 0)
        return carry

    steps = hops - second
    lax.fori_loop(0, steps, steady, 0)
    for g in range(min(steps, chunks), chunks):
        multiply_own(g)
        multiply_peer(g)

    def settle(q, carry):
        for direction in (0, 1):
            link(direction, q, 0).wait_send()
        product_copy(q).wait_send()
        return carry

    lax.fori_loop(0, hops - 1, settle, 0)
    for g in range(chunks):
        peer_copy(g).wait_send()
    lax.fori_loop(taken(steps), hops, take, 0)
    lax.fori_loop(hops - 1, hops, settle, 0)


def solution(mesh):
    n_prow, n_pcol = mesh.shape["prow"], mesh.shape["pcol"]
    n_x, n_z, parts, chunks, early = n_prow // 2, n_pcol // 2, 8, 4, (1, 4)

    def local(slab, panel, pivots, inv_lower, inv_upper):
        (row_count, columns), (rows, nb) = slab.shape, panel.shape
        half = columns // 2
        hops = parts * (n_z - 1) // 2
        pair = 2 * rows // parts
        hbm = pl.BlockSpec(memory_space=pltpu.HBM)
        dma = pltpu.SemaphoreType.DMA
        flops = 2 * row_count * nb * (nb + columns)
        return pl.pallas_call(
            functools.partial(kernel, n_x, n_z, parts, chunks, early),
            out_shape=pltpu.VMEM(slab.shape, slab.dtype),
            in_specs=[
                hbm,
                hbm,
                pl.BlockSpec(memory_space=pltpu.SMEM),
                pl.BlockSpec(memory_space=pltpu.VMEM),
                hbm,
                hbm,
            ],
            out_specs=pl.BlockSpec(memory_space=pltpu.VMEM),
            scratch_shapes=[
                pltpu.VMEM((n_z, rows, nb), F32),
                pltpu.VMEM((rows, nb), F32),
                pltpu.VMEM((2, hops, pair, nb), BF16),
                pltpu.VMEM((2, rows, nb), BF16),
                pltpu.VMEM((hops, pair, columns), F32),
                pltpu.VMEM((hops, pair, columns), F32),
                pltpu.VMEM((nb, nb), F32),
                pltpu.VMEM((nb, nb), F32),
                pltpu.VMEM((2, nb, nb), BF16),
                pltpu.VMEM((2, nb, half), F32),
                pltpu.VMEM((nb, half), F32),
                pltpu.VMEM((nb, half), F32),
                pltpu.VMEM((max(n_x - 1, 1), nb, half), F32),
                pltpu.VMEM((nb, half), F32),
                pltpu.VMEM((4, nb, half), F32),
                pltpu.VMEM((2, nb, 2 * columns), BF16),
                dma((4,)),
                dma((2 * hops,)),
                dma((2 * hops,)),
                dma((hops,)),
                dma((hops,)),
                dma,
                dma,
                dma((max(n_x - 1, 1),)),
                dma((max(n_x - 1, 1),)),
                dma((3,)),
                dma((3,)),
                dma((chunks,)),
                dma((chunks,)),
            ],
            compiler_params=pltpu.CompilerParams(
                collective_id=0, has_side_effects=True, vmem_limit_bytes=32 * 2**20
            ),
            cost_estimate=pl.CostEstimate(
                flops=flops, bytes_accessed=8 * slab.size, transcendentals=0
            ),
        )(
            *(pltpu.with_memory_space_constraint(a, pltpu.HBM) for a in (slab, panel)),
            pivots,
            pivots.reshape(1, nb),
            *(pltpu.with_memory_space_constraint(a, pltpu.HBM) for a in (inv_lower, inv_upper)),
        )

    return jax.shard_map(
        local,
        mesh=mesh,
        in_specs=(P("prow", "pcol"), P(("prow", "pcol"), None), P(), P(), P()),
        out_specs=P("prow", "pcol"),
        check_vma=False,
    )
```

```python
import functools

import jax
import jax.numpy as jnp
from jax import lax
from jax.experimental import pallas as pl
from jax.experimental.pallas import tpu as pltpu
from jax.sharding import PartitionSpec as P

MESH = pl.DeviceIdType.MESH
HIGHEST = lax.Precision.HIGHEST
F32 = jnp.float32
BF16 = jnp.bfloat16


def dot(a, b):
    return jnp.dot(a, b, precision=HIGHEST, preferred_element_type=F32)


def split(a):
    high = a.astype(BF16)
    return high, (a - high.astype(F32)).astype(BF16)


def dot_split(a_high, a_low, b_high, b_low):
    rows = a_high.shape[0]
    both = jnp.dot(
        jnp.concatenate([a_high, a_low], axis=0), b_high, preferred_element_type=F32
    )
    cross = jnp.dot(a_high, b_low, preferred_element_type=F32)
    return both[:rows] + (both[rows:] + cross)


def kernel(
    n_x, n_z, parts, chunks, ahead, early,
    slab_ref, panel_ref, pivots_ref, pivot_row_ref, inv_lower_ref, inv_upper_ref,
    out_ref,
    raw, raw_peer, lower, stage, landed, inv_lower, inv_upper, inv_split,
    picked, partner_part, chip_sum, from_x, total, halves, upper, pivots, pivot_row,
    load_sem, link_send, link_recv, product_send, product_recv,
    pick_send, pick_recv, x_send, x_recv, half_send, half_recv, peer_send, peer_recv,
):
    slab = out_ref
    prow = lax.axis_index("prow")
    pcol = lax.axis_index("pcol")
    x, core = prow // 2, prow % 2
    z, y = pcol // 2, pcol % 2
    rows, nb = panel_ref.shape
    piece, chunk = rows // parts, rows // chunks
    row_count, columns = slab_ref.shape
    half = columns // 2
    first_row = prow * row_count
    hops = parts * (n_z - 1)
    partner = {"prow": x * 2 + 1 - core}
    peer = {"pcol": z * 2 + 1 - y}
    left = {"pcol": (z - 1) * 2 + y}
    right = {"pcol": (z + 1) * 2 + y}
    has_left, has_right = z > 0, z < n_z - 1
    others = [{"prow": lax.rem(x + o, n_x) * 2 + core} for o in range(1, n_x)]

    barrier = pltpu.get_barrier_semaphore()
    for exists, device in ((has_left, left), (has_right, right)):
        @pl.when(exists)
        def _():
            pl.semaphore_signal(barrier, inc=1, device_id=device, device_id_type=MESH)
    fixed = [peer] + others + [partner]
    for device in fixed:
        pl.semaphore_signal(barrier, inc=1, device_id=device, device_id_type=MESH)

    panel_load = pltpu.make_async_copy(panel_ref, raw.at[z], load_sem.at[0])
    slab_load = pltpu.make_async_copy(slab_ref, slab, load_sem.at[1])
    upper_load = pltpu.make_async_copy(inv_upper_ref, inv_upper, load_sem.at[2])
    lower_load = pltpu.make_async_copy(inv_lower_ref, inv_lower, load_sem.at[3])
    pivot_load = pltpu.make_async_copy(pivots_ref, pivots, load_sem.at[4])
    pivot_row_load = pltpu.make_async_copy(pivot_row_ref, pivot_row, load_sem.at[5])
    for load in (panel_load, pivot_load, slab_load, pivot_row_load, upper_load, lower_load):
        load.start()

    def remote(source, target, send_sem, recv_sem, device):
        return pltpu.make_async_remote_copy(
            src_ref=source, dst_ref=target, send_sem=send_sem, recv_sem=recv_sem,
            device_id=device, device_id_type=MESH,
        )

    def span_of(start, count):
        return pl.ds(pl.multiple_of(start, 8), count)

    def place(direction, q, away):
        distance = q // parts + away
        block = z - distance if direction == 0 else z + distance
        return block, (q % parts) * piece

    def sends(direction, q):
        block, _ = place(direction, q, 0)
        return has_right & (block >= 0) if direction == 0 else has_left & (block < n_z)

    def receives(direction, q):
        block, _ = place(direction, q, 1)
        return block >= 0 if direction == 0 else block < n_z

    def link(direction, q, away):
        block, start = place(direction, q, away)
        spot = raw.at[block, span_of(start, piece)]
        index = direction * hops + q
        return remote(
            spot, spot, link_send.at[index], link_recv.at[index],
            right if direction == 0 else left,
        )

    def peer_copy(g):
        span = span_of(g * chunk, chunk)
        return remote(
            raw.at[z, span], raw_peer.at[span], peer_send.at[g], peer_recv.at[g], peer
        )

    panel_load.wait()
    n_peers = len(fixed) + has_left.astype(jnp.int32) + has_right.astype(jnp.int32)
    pl.semaphore_wait(barrier, n_peers)
    for q in range(parts):
        for direction in (0, 1):
            @pl.when(sends(direction, q))
            def _():
                link(direction, q, 0).start()
    for g in range(ahead[0]):
        peer_copy(g).start()

    pivot_load.wait()
    slab_load.wait()

    def pick(k, carry):
        local = pivots[k] - first_row
        inside = (local >= 0) & (local < row_count)
        row = slab[pl.ds(jnp.where(inside, local, 0), 1), :]
        row = jnp.where(inside, row, 0.0)
        picked[0, pl.ds(k, 1), :] = row[:, :half]
        picked[1, pl.ds(k, 1), :] = row[:, half:]
        return carry

    lax.fori_loop(0, nb, pick, 0, unroll=8)

    pick_copy = remote(picked.at[1 - core], partner_part, pick_send, pick_recv, partner)
    pick_copy.start()
    pivot_row_load.wait()
    upper_load.wait()
    lower_load.wait()
    inv_split[0], inv_split[1] = split(inv_upper[...])
    pick_copy.wait()
    chip_sum[...] = picked[core] + partner_part[...]
    x_copies = [
        remote(chip_sum, from_x.at[i], x_send.at[i], x_recv.at[i], device)
        for i, device in enumerate(others)
    ]
    for copy in x_copies:
        copy.start()

    def pivot_hits(start, count):
        ids = first_row + start + lax.broadcasted_iota(jnp.int32, (count, nb), 0)
        return jnp.where(ids == pivot_row[...], 1.0, 0.0)

    def is_pivot(hits):
        return jnp.max(hits, axis=1, keepdims=True) > 0.0

    def solve(rows_in, hits):
        high, low = split(rows_in)
        solved = dot_split(high, low, inv_split[0], inv_split[1])
        return split(jnp.where(is_pivot(hits), -hits, solved))

    def clear(i, carry):
        start = i * chunk
        span = span_of(start, chunk)
        slab[span, :] = jnp.where(
            is_pivot(pivot_hits(start, chunk)), 0.0, slab[span, :]
        )
        return carry

    lax.fori_loop(0, row_count // chunk, clear, 0)

    def solve_rows(block, start, count):
        span = span_of(start, count)
        hits = pivot_hits((block * 2 + y) * rows + start, count)
        high, low = solve(raw[block, span, :], hits)
        lower[0, block, span, :] = high
        lower[1, block, span, :] = low

    def prepare(q, carry):
        for direction in (0, 1):
            @pl.when(receives(direction, q))
            def _():
                link(direction, q, 1).wait_recv()

            @pl.when(receives(direction, q) & sends(direction, q + parts))
            def _():
                link(direction, q + parts, 0).start()

            @pl.when(receives(direction, q))
            def _():
                solve_rows(*place(direction, q, 1), piece)
        return carry

    first, second = min(early[0], hops), min(early[1], hops)
    lax.fori_loop(0, first, prepare, 0)

    for copy in x_copies:
        copy.wait()
    summed = chip_sum[...]
    for o in range(1, n_x):
        summed = summed + from_x[o - 1]
    total[...] = summed
    halves[core] = dot(inv_lower[...], total[...])
    to_peer = remote(
        halves.at[core], halves.at[2 + core], half_send.at[0], half_recv.at[0], peer
    )
    to_partner = remote(
        halves.at[core], halves.at[core], half_send.at[1], half_recv.at[1], partner
    )
    to_peer.start()
    to_partner.start()
    for g in range(ahead[0], ahead[1]):
        peer_copy(g).start()

    def solve_own(g, carry):
        solve_rows(z, g * chunk, chunk)
        return carry

    lax.fori_loop(0, chunks, solve_own, 0)
    lax.fori_loop(first, second, prepare, 0)

    to_peer.wait()
    onward = remote(
        halves.at[2 + core], halves.at[2 + core], half_send.at[2], half_recv.at[2], partner
    )
    onward.start()
    to_partner.wait()

    def split_upper(i):
        span = slice(i * half, (i + 1) * half)
        upper[0, :, span], upper[1, :, span] = split(halves[i])

    split_upper(0)
    split_upper(1)
    onward.wait()
    split_upper(2)
    split_upper(3)

    def product_copy(direction, q):
        block, start = place(direction, q, 1)
        span = span_of(start, piece)
        index = direction * hops + q
        return remote(
            stage.at[block, span], landed.at[block, span],
            product_send.at[index], product_recv.at[index], peer,
        )

    def subtract(block, side, start, count, product):
        span = span_of((block * 2 + side) * rows + start, count)
        slab[span, :] = slab[span, :] - product

    def multiply(q, carry):
        for direction in (0, 1):
            @pl.when(receives(direction, q))
            def _():
                block, start = place(direction, q, 1)
                span = span_of(start, piece)
                products = dot_split(
                    lower[0, block, span, :], lower[1, block, span, :],
                    upper[0], upper[1],
                )
                stage[block, span, :] = products[:, columns:]
                product_copy(direction, q).start()
                subtract(block, y, start, piece, products[:, :columns])
        return carry

    def take(q, carry):
        for direction in (0, 1):
            @pl.when(receives(direction, q))
            def _():
                block, start = place(direction, q, 1)
                product_copy(direction, q).wait_recv()
                subtract(
                    block, 1 - y, start, piece, landed[block, span_of(start, piece), :]
                )
        return carry

    def multiply_own(g, carry):
        span = span_of(g * chunk, chunk)
        product = dot_split(
            lower[0, z, span, :], lower[1, z, span, :],
            upper[0, :, :columns], upper[1, :, :columns],
        )
        subtract(z, y, g * chunk, chunk, product)
        return carry

    def multiply_peer(g, carry):
        peer_copy(g).wait_recv()
        start = g * chunk
        hits = pivot_hits((z * 2 + 1 - y) * rows + start, chunk)
        high, low = solve(raw_peer[span_of(start, chunk), :], hits)
        product = dot_split(high, low, upper[0, :, :columns], upper[1, :, :columns])
        subtract(z, 1 - y, start, chunk, product)
        return carry

    lax.fori_loop(0, second, multiply, 0)

    steps = hops - second
    middle = steps // 2

    def taken(q):
        return jnp.clip(2 * q - hops + 1, 0, q)

    def reached(i, start):
        return jnp.clip(i - start, 0, chunks)

    def steady(i, carry):
        q = second + i
        prepare(q, 0)
        multiply(q, 0)
        last = ahead[1] + reached(i, 0)

        @pl.when(last < chunks)
        def _():
            peer_copy(last).start()

        lax.fori_loop(reached(i, 0), reached(i + 1, 0), multiply_own, 0)
        lax.fori_loop(reached(i, middle), reached(i + 1, middle), multiply_peer, 0)
        lax.fori_loop(jnp.where(i > 0, taken(q - 1), 0), taken(q), take, 0)
        return carry

    lax.fori_loop(0, steps, steady, 0)
    for g in range(min(ahead[1] + steps, chunks), chunks):
        peer_copy(g).start()
    lax.fori_loop(min(steps, chunks), chunks, multiply_own, 0)
    lax.fori_loop(min(steps - middle, chunks), chunks, multiply_peer, 0)

    def settle(q, carry):
        for direction in (0, 1):
            @pl.when(sends(direction, q))
            def _():
                link(direction, q, 0).wait_send()

            @pl.when(receives(direction, q))
            def _():
                product_copy(direction, q).wait_send()
        return carry

    lax.fori_loop(0, hops - 1, settle, 0)
    for g in range(chunks):
        peer_copy(g).wait_send()
    lax.fori_loop(hops - 1 if steps else 0, hops, take, 0)
    lax.fori_loop(hops - 1, hops, settle, 0)


def solution(mesh):
    n_prow, n_pcol = mesh.shape["prow"], mesh.shape["pcol"]
    n_x, n_z = n_prow // 2, n_pcol // 2
    parts, chunks, ahead, early = 8, 8, (5, 6), (2, 5)

    def local(slab, panel, pivots, inv_lower, inv_upper):
        (row_count, columns), (rows, nb) = slab.shape, panel.shape
        half = columns // 2
        hops = parts * (n_z - 1)
        hbm = pl.BlockSpec(memory_space=pltpu.HBM)
        dma = pltpu.SemaphoreType.DMA
        flops = 2 * row_count * nb * (nb + columns)
        return pl.pallas_call(
            functools.partial(kernel, n_x, n_z, parts, chunks, ahead, early),
            out_shape=pltpu.VMEM(slab.shape, slab.dtype),
            in_specs=[
                hbm,
                hbm,
                hbm,
                hbm,
                hbm,
                hbm,
            ],
            out_specs=pl.BlockSpec(memory_space=pltpu.VMEM),
            scratch_shapes=[
                pltpu.VMEM((n_z, rows, nb), F32),
                pltpu.VMEM((rows, nb), F32),
                pltpu.VMEM((2, n_z, rows, nb), BF16),
                pltpu.VMEM((n_z, rows, columns), F32),
                pltpu.VMEM((n_z, rows, columns), F32),
                pltpu.VMEM((nb, nb), F32),
                pltpu.VMEM((nb, nb), F32),
                pltpu.VMEM((2, nb, nb), BF16),
                pltpu.VMEM((2, nb, half), F32),
                pltpu.VMEM((nb, half), F32),
                pltpu.VMEM((nb, half), F32),
                pltpu.VMEM((max(n_x - 1, 1), nb, half), F32),
                pltpu.VMEM((nb, half), F32),
                pltpu.VMEM((4, nb, half), F32),
                pltpu.VMEM((2, nb, 2 * columns), BF16),
                pltpu.SMEM((nb,), jnp.int32),
                pltpu.VMEM((1, nb), jnp.int32),
                dma((6,)),
                dma((2 * hops,)),
                dma((2 * hops,)),
                dma((2 * hops,)),
                dma((2 * hops,)),
                dma,
                dma,
                dma((max(n_x - 1, 1),)),
                dma((max(n_x - 1, 1),)),
                dma((3,)),
                dma((3,)),
                dma((chunks,)),
                dma((chunks,)),
            ],
            compiler_params=pltpu.CompilerParams(
                collective_id=0, has_side_effects=True, vmem_limit_bytes=32 * 2**20
            ),
            cost_estimate=pl.CostEstimate(
                flops=flops, bytes_accessed=8 * slab.size, transcendentals=0
            ),
        )(
            *(
                pltpu.with_memory_space_constraint(a, pltpu.HBM)
                for a in (slab, panel, pivots, pivots.reshape(1, nb), inv_lower, inv_upper)
            )
        )

    return jax.shard_map(
        local,
        mesh=mesh,
        in_specs=(P("prow", "pcol"), P(("prow", "pcol"), None), P(), P(), P()),
        out_specs=P("prow", "pcol"),
        check_vma=False,
    )
```

```python
import functools

import jax
import jax.numpy as jnp
from jax import lax
from jax.experimental import pallas as pl
from jax.experimental.pallas import tpu as pltpu
from jax.sharding import PartitionSpec as P

MESH = pl.DeviceIdType.MESH
HIGHEST = lax.Precision.HIGHEST
F32 = jnp.float32
BF16 = jnp.bfloat16


def dot(a, b):
    return jnp.dot(a, b, precision=HIGHEST, preferred_element_type=F32)


def split(a):
    high = a.astype(BF16)
    return high, (a - high.astype(F32)).astype(BF16)


def dot_split(a_high, a_low, b_high, b_low):
    rows = a_high.shape[0]
    both = jnp.dot(
        jnp.concatenate([a_high, a_low], axis=0), b_high, preferred_element_type=F32
    )
    cross = jnp.dot(a_high, b_low, preferred_element_type=F32)
    return both[:rows] + (both[rows:] + cross)


def kernel(
    n_x, n_z, early,
    slab_ref, panel_ref, pivots_ref, pivot_row_ref, inv_lower_ref, inv_upper_ref,
    out_ref,
    raw, raw_peer, lower, stage, landed, inv_lower, inv_upper, inv_split,
    picked, partner_part, chip_sum, from_x, total, halves, upper, pivots, pivot_row,
    guest, guest_split, direct, direct_landed,
    load_sem, link_send, link_recv, product_send, product_recv,
    pick_send, pick_recv, x_send, x_recv, half_send, half_recv, peer_send, peer_recv,
    guest_send, guest_recv, direct_send, direct_recv,
):
    slab = out_ref
    prow = lax.axis_index("prow")
    pcol = lax.axis_index("pcol")
    x, core = prow // 2, prow % 2
    z, y = pcol // 2, pcol % 2
    rows, nb = panel_ref.shape
    unit = rows // 8
    pieces = [(0, 2 * unit), (2 * unit, 2 * unit), (4 * unit, 2 * unit)]
    pieces += [(6 * unit, unit), (7 * unit, unit)]
    final = len(pieces) - 1
    peer_pieces = [(0, 2 * unit), (2 * unit, 2 * unit), (4 * unit, unit)]
    peer_pieces += [(5 * unit, unit), (6 * unit, 2 * unit)]
    chunk = 2 * unit
    row_count, columns = slab_ref.shape
    half = columns // 2
    first_row = prow * row_count
    partner = {"prow": x * 2 + 1 - core}
    peer = {"pcol": z * 2 + 1 - y}
    left = {"pcol": (z - 1) * 2 + y}
    right = {"pcol": (z + 1) * 2 + y}
    has_left, has_right = z > 0, z < n_z - 1
    others = [{"prow": lax.rem(x + o, n_x) * 2 + core} for o in range(1, n_x)]

    barrier = pltpu.get_barrier_semaphore()
    for exists, device in ((has_left, left), (has_right, right)):
        @pl.when(exists)
        def _():
            pl.semaphore_signal(barrier, inc=1, device_id=device, device_id_type=MESH)
    fixed = [peer] + others + [partner]
    for device in fixed:
        pl.semaphore_signal(barrier, inc=1, device_id=device, device_id_type=MESH)

    panel_load = pltpu.make_async_copy(panel_ref, raw.at[z], load_sem.at[0])
    slab_load = pltpu.make_async_copy(slab_ref, slab, load_sem.at[1])
    upper_load = pltpu.make_async_copy(inv_upper_ref, inv_upper, load_sem.at[2])
    lower_load = pltpu.make_async_copy(inv_lower_ref, inv_lower, load_sem.at[3])
    pivot_load = pltpu.make_async_copy(pivots_ref, pivots, load_sem.at[4])
    pivot_row_load = pltpu.make_async_copy(pivot_row_ref, pivot_row, load_sem.at[5])
    for load in (panel_load, pivot_load, slab_load, pivot_row_load, upper_load, lower_load):
        load.start()

    def remote(source, target, send_sem, recv_sem, device):
        return pltpu.make_async_remote_copy(
            src_ref=source, dst_ref=target, send_sem=send_sem, recv_sem=recv_sem,
            device_id=device, device_id_type=MESH,
        )

    def span_of(start, count):
        return pl.ds(pl.multiple_of(start, 8), count)

    def block_at(direction, distance):
        return z - distance if direction == 0 else z + distance

    def receives(direction, distance):
        block = block_at(direction, distance)
        return block >= 0 if direction == 0 else block < n_z

    def sends(direction, distance):
        exists = has_right if direction == 0 else has_left
        return exists & receives(direction, distance)

    def guest_of(direction):
        return z == n_z - 1 if direction == 0 else z == 0

    def host_of(direction):
        return z == n_z - 2 if direction == 0 else z == 1

    def comes(direction, distance, g):
        exists = receives(direction, distance)
        if g == final:
            exists &= ~(guest_of(direction) & (distance == 1))
        return exists

    def goes(direction, g):
        exists = sends(direction, 0)
        if g == final:
            exists &= ~host_of(direction)
        return exists

    def link(direction, distance, g):
        block = block_at(direction, distance)
        spot = raw.at[block, pl.ds(*pieces[g])]
        return remote(
            spot, spot, link_send.at[direction * n_z + distance],
            link_recv.at[block * len(pieces) + g], right if direction == 0 else left,
        )

    def peer_copy(i):
        span = pl.ds(*peer_pieces[i])
        return remote(
            raw.at[z, span], raw_peer.at[span], peer_send.at[i], peer_recv.at[i], peer
        )

    panel_load.wait()
    n_peers = len(fixed) + has_left.astype(jnp.int32) + has_right.astype(jnp.int32)
    pl.semaphore_wait(barrier, n_peers)
    for g in range(len(pieces)):
        for direction in (0, 1):
            @pl.when(goes(direction, g))
            def _():
                link(direction, 0, g).start()
    for i in range(3):
        peer_copy(i).start()

    pivot_load.wait()
    slab_load.wait()

    def pick(k, carry):
        local = pivots[k] - first_row
        inside = (local >= 0) & (local < row_count)
        row = slab[pl.ds(jnp.where(inside, local, 0), 1), :]
        row = jnp.where(inside, row, 0.0)
        picked[0, pl.ds(k, 1), :] = row[:, :half]
        picked[1, pl.ds(k, 1), :] = row[:, half:]
        return carry

    lax.fori_loop(0, nb, pick, 0, unroll=8)

    pick_copy = remote(picked.at[1 - core], partner_part, pick_send, pick_recv, partner)
    pick_copy.start()
    pivot_row_load.wait()
    upper_load.wait()
    lower_load.wait()
    inv_split[0], inv_split[1] = split(inv_upper[...])
    pick_copy.wait()
    chip_sum[...] = picked[core] + partner_part[...]
    x_copies = [
        remote(chip_sum, from_x.at[i], x_send.at[i], x_recv.at[i], device)
        for i, device in enumerate(others)
    ]
    for copy in x_copies:
        copy.start()

    def pivot_hits(start, count):
        ids = first_row + start + lax.broadcasted_iota(jnp.int32, (count, nb), 0)
        return jnp.where(ids == pivot_row[...], 1.0, 0.0)

    def is_pivot(hits):
        return jnp.max(hits, axis=1, keepdims=True) > 0.0

    def solve(rows_in, hits):
        high, low = split(rows_in)
        solved = dot_split(high, low, inv_split[0], inv_split[1])
        return split(jnp.where(is_pivot(hits), -hits, solved))

    def clear(i, carry):
        start = i * 2 * chunk
        span = span_of(start, 2 * chunk)
        slab[span, :] = jnp.where(
            is_pivot(pivot_hits(start, 2 * chunk)), 0.0, slab[span, :]
        )
        return carry

    lax.fori_loop(0, row_count // (2 * chunk), clear, 0)

    def solve_rows(block, start, count):
        span = span_of(start, count)
        hits = pivot_hits((block * 2 + y) * rows + start, count)
        high, low = solve(raw[block, span, :], hits)
        lower[0, block, span, :] = high
        lower[1, block, span, :] = low

    def prepare(distance, g):
        for direction in (0, 1):
            arrives = comes(direction, distance, g)

            @pl.when(arrives)
            def _():
                link(direction, distance, g).wait_recv()

            @pl.when(arrives & sends(direction, distance))
            def _():
                link(direction, distance, g).start()

            @pl.when(arrives)
            def _():
                solve_rows(block_at(direction, distance), *pieces[g])

    for g in range(early[0]):
        prepare(1, g)

    for copy in x_copies:
        copy.wait()
    summed = chip_sum[...]
    for o in range(1, n_x):
        summed = summed + from_x[o - 1]
    total[...] = summed
    halves[core] = dot(inv_lower[...], total[...])
    to_peer = remote(
        halves.at[core], halves.at[2 + core], half_send.at[0], half_recv.at[0], peer
    )
    to_partner = remote(
        halves.at[core], halves.at[core], half_send.at[1], half_recv.at[1], partner
    )
    to_peer.start()
    to_partner.start()
    peer_copy(3).start()

    def solve_own(g, carry):
        solve_rows(z, g * chunk, chunk)
        return carry

    lax.fori_loop(0, rows // chunk, solve_own, 0)
    for g in range(early[0], early[1]):
        prepare(1, g)

    to_peer.wait()
    onward = remote(
        halves.at[2 + core], halves.at[2 + core], half_send.at[2], half_recv.at[2], partner
    )
    onward.start()
    to_partner.wait()

    def split_upper(i):
        span = slice(i * half, (i + 1) * half)
        upper[0, :, span], upper[1, :, span] = split(halves[i])

    split_upper(0)
    split_upper(1)
    onward.wait()
    split_upper(2)
    split_upper(3)

    def guest_copy(direction):
        return remote(
            halves.at[0:2], guest.at[direction], guest_send.at[direction],
            guest_recv.at[direction], left if direction == 0 else right,
        )

    def direct_copy(direction):
        return remote(
            direct.at[direction], direct_landed, direct_send.at[direction],
            direct_recv, right if direction == 0 else left,
        )

    for direction in (0, 1):
        @pl.when(guest_of(direction))
        def _():
            guest_copy(direction).start()

    def product_copy(direction, distance, g):
        block = block_at(direction, distance)
        span = pl.ds(*pieces[g])
        return remote(
            stage.at[block, span], landed.at[block, span],
            product_send.at[block], product_recv.at[block * len(pieces) + g], peer,
        )

    def subtract(block, side, start, count, product):
        span = span_of((block * 2 + side) * rows + start, count)
        slab[span, :] = slab[span, :] - product

    def multiply(distance, g):
        start, count = pieces[g]
        span = pl.ds(start, count)
        for direction in (0, 1):
            @pl.when(comes(direction, distance, g))
            def _():
                block = block_at(direction, distance)
                products = dot_split(
                    lower[0, block, span, :], lower[1, block, span, :],
                    upper[0], upper[1],
                )
                stage[block, span, :] = products[:, columns:]
                product_copy(direction, distance, g).start()
                subtract(block, y, start, count, products[:, :columns])

    def take(distance, g):
        start, count = pieces[g]
        for direction in (0, 1):
            @pl.when(comes(direction, distance, g))
            def _():
                block = block_at(direction, distance)
                product_copy(direction, distance, g).wait_recv()
                subtract(
                    block, 1 - y, start, count, landed[block, pl.ds(start, count), :]
                )

    def multiply_own(i, carry):
        span = span_of(i * chunk, chunk)
        product = dot_split(
            lower[0, z, span, :], lower[1, z, span, :],
            upper[0, :, :columns], upper[1, :, :columns],
        )
        subtract(z, y, i * chunk, chunk, product)
        return carry

    def solve_peer(start, count):
        hits = pivot_hits((z * 2 + 1 - y) * rows + start, count)
        return solve(raw_peer[pl.ds(start, count), :], hits)

    def multiply_peer(i):
        for c in ((0,), (1,), (2, 3), (4,))[i]:
            peer_copy(c).wait_recv()
        high, low = solve_peer(i * chunk, chunk)
        product = dot_split(high, low, upper[0, :, :columns], upper[1, :, :columns])
        subtract(z, 1 - y, i * chunk, chunk, product)

    def serve():
        for direction in (0, 1):
            @pl.when(host_of(direction))
            def _():
                guest_copy(direction).wait_recv()
                for i in (0, 1):
                    span = slice(i * half, (i + 1) * half)
                    guest_split[0, :, span], guest_split[1, :, span] = split(
                        guest[direction, i]
                    )
                start, count = pieces[final]
                high, low = solve_peer(start, count)
                direct[direction] = dot_split(
                    jnp.concatenate([lower[0, z, pl.ds(start, count), :], high], axis=0),
                    jnp.concatenate([lower[1, z, pl.ds(start, count), :], low], axis=0),
                    guest_split[0], guest_split[1],
                )
                direct_copy(direction).start()

    for g in range(early[1]):
        multiply(1, g)
    peer_copy(4).start()
    for g in range(early[1], len(pieces)):
        prepare(1, g)
        multiply(1, g)
        lax.fori_loop(2 * (g - early[1]), 2 * (g - early[1]) + 2, multiply_own, 0)

    def step(distance, final_step):
        for g in range(len(pieces)):
            prepare(distance, g)
            multiply(distance, g)
            if isinstance(distance, int) and not final_step and g < 4:
                multiply_peer(g)
            take(distance - 1, g)
            if final_step and g >= 2:
                take(distance, g - 2)

    if n_z <= 3:
        for i in range(4):
            multiply_peer(i)
    if n_z > 3:
        step(2, False)
        lax.fori_loop(3, n_z - 1, lambda d, c: (step(d, False), c)[1], 0)
    serve()
    if n_z > 2:
        step(n_z - 1, True)

    def settle_products(direction, distance):
        block = block_at(direction, distance)

        def wait(count):
            span = pl.ds(0, count)
            remote(
                stage.at[block, span], landed.at[block, span],
                product_send.at[block], product_recv.at[0], peer,
            ).wait_send()

        whole = receives(direction, distance)
        short = guest_of(direction) & (distance == 1)
        pl.when(whole & ~short)(lambda: wait(rows))
        pl.when(whole & short)(lambda: wait(pieces[final][0]))

    def settle_links(direction, distance):
        block = block_at(direction, distance)

        def wait(count):
            spot = raw.at[block, pl.ds(0, count)]
            remote(
                spot, spot, link_send.at[direction * n_z + distance], link_recv.at[0],
                right if direction == 0 else left,
            ).wait_send()

        whole = sends(direction, distance)
        short = host_of(direction) & (distance == 0)
        pl.when(whole & ~short)(lambda: wait(rows))
        pl.when(whole & short)(lambda: wait(pieces[final][0]))

    def settle(distance, carry):
        for direction in (0, 1):
            settle_links(direction, distance)
        return carry

    lax.fori_loop(0, n_z - 1, settle, 0)
    for i in range(len(peer_pieces)):
        peer_copy(i).wait_send()
    for direction in (0, 1):
        @pl.when(guest_of(direction))
        def _():
            guest_copy(direction).wait_send()
    for g in range(final - 1 if n_z > 2 else 0, len(pieces)):
        take(n_z - 1, g)

    def settle_late(distance, carry):
        for direction in (0, 1):
            settle_products(direction, distance)
        return carry

    lax.fori_loop(1, n_z, settle_late, 0)
    for direction in (0, 1):
        @pl.when(host_of(direction))
        def _():
            direct_copy(direction).wait_send()

        @pl.when(guest_of(direction))
        def _():
            direct_copy(direction).wait_recv()
            start, count = pieces[final]
            block = block_at(direction, 1)
            subtract(block, y, start, count, direct_landed[:count])
            subtract(block, 1 - y, start, count, direct_landed[count:])


def solution(mesh):
    n_prow, n_pcol = mesh.shape["prow"], mesh.shape["pcol"]
    n_x, n_z, n_pieces, early = n_prow // 2, n_pcol // 2, 5, (1, 3)

    def local(slab, panel, pivots, inv_lower, inv_upper):
        (row_count, columns), (rows, nb) = slab.shape, panel.shape
        half = columns // 2
        pair = rows // 4
        hbm = pl.BlockSpec(memory_space=pltpu.HBM)
        dma = pltpu.SemaphoreType.DMA
        flops = 2 * row_count * nb * (nb + columns)
        return pl.pallas_call(
            functools.partial(kernel, n_x, n_z, early),
            out_shape=pltpu.VMEM(slab.shape, slab.dtype),
            in_specs=[
                hbm,
                hbm,
                hbm,
                hbm,
                hbm,
                hbm,
            ],
            out_specs=pl.BlockSpec(memory_space=pltpu.VMEM),
            scratch_shapes=[
                pltpu.VMEM((n_z, rows, nb), F32),
                pltpu.VMEM((rows, nb), F32),
                pltpu.VMEM((2, n_z, rows, nb), BF16),
                pltpu.VMEM((n_z, rows, columns), F32),
                pltpu.VMEM((n_z, rows, columns), F32),
                pltpu.VMEM((nb, nb), F32),
                pltpu.VMEM((nb, nb), F32),
                pltpu.VMEM((2, nb, nb), BF16),
                pltpu.VMEM((2, nb, half), F32),
                pltpu.VMEM((nb, half), F32),
                pltpu.VMEM((nb, half), F32),
                pltpu.VMEM((max(n_x - 1, 1), nb, half), F32),
                pltpu.VMEM((nb, half), F32),
                pltpu.VMEM((4, nb, half), F32),
                pltpu.VMEM((2, nb, 2 * columns), BF16),
                pltpu.SMEM((nb,), jnp.int32),
                pltpu.VMEM((1, nb), jnp.int32),
                pltpu.VMEM((2, 2, nb, half), F32),
                pltpu.VMEM((2, nb, columns), BF16),
                pltpu.VMEM((2, pair, columns), F32),
                pltpu.VMEM((pair, columns), F32),
                dma((6,)),
                dma((2 * n_z,)),
                dma((n_pieces * n_z,)),
                dma((n_z,)),
                dma((n_pieces * n_z,)),
                dma,
                dma,
                dma((max(n_x - 1, 1),)),
                dma((max(n_x - 1, 1),)),
                dma((3,)),
                dma((3,)),
                dma((5,)),
                dma((5,)),
                dma((2,)),
                dma((2,)),
                dma((2,)),
                dma,
            ],
            compiler_params=pltpu.CompilerParams(
                collective_id=0, has_side_effects=True, vmem_limit_bytes=32 * 2**20
            ),
            cost_estimate=pl.CostEstimate(
                flops=flops, bytes_accessed=8 * slab.size, transcendentals=0
            ),
        )(
            *(
                pltpu.with_memory_space_constraint(a, pltpu.HBM)
                for a in (slab, panel, pivots, pivots.reshape(1, nb), inv_lower, inv_upper)
            )
        )

    return jax.shard_map(
        local,
        mesh=mesh,
        in_specs=(P("prow", "pcol"), P(("prow", "pcol"), None), P(), P(), P()),
        out_specs=P("prow", "pcol"),
        check_vma=False,
    )
```

```python
import functools

import jax
import jax.numpy as jnp
from jax import lax
from jax.experimental import pallas as pl
from jax.experimental.pallas import tpu as pltpu
from jax.sharding import PartitionSpec as P

MESH = pl.DeviceIdType.MESH
HIGHEST = lax.Precision.HIGHEST
F32 = jnp.float32
BF16 = jnp.bfloat16


def dot(a, b):
    return jnp.dot(a, b, precision=HIGHEST, preferred_element_type=F32)


def split(a):
    high = a.astype(BF16)
    return high, (a - high.astype(F32)).astype(BF16)


def dot_split(a_high, a_low, b_high, b_low):
    rows = a_high.shape[0]
    both = jnp.dot(
        jnp.concatenate([a_high, a_low], axis=0), b_high, preferred_element_type=F32
    )
    cross = jnp.dot(a_high, b_low, preferred_element_type=F32)
    return both[:rows] + (both[rows:] + cross)


def kernel(
    n_x, n_z, early,
    slab_ref, panel_ref, pivots_ref, pivot_row_ref, inv_lower_ref, inv_upper_ref,
    out_ref,
    raw, raw_peer, lower, stage, landed, inv_lower, inv_upper, inv_split,
    picked, partner_part, chip_sum, from_x, total, halves, upper, pivots, pivot_row,
    guest, guest_split, direct, direct_landed,
    load_sem, link_send, link_recv, product_send, product_recv,
    pick_send, pick_recv, x_send, x_recv, half_send, half_recv, peer_send, peer_recv,
    guest_send, guest_recv, direct_send, direct_recv,
):
    slab = out_ref
    prow = lax.axis_index("prow")
    pcol = lax.axis_index("pcol")
    x, core = prow // 2, prow % 2
    z, y = pcol // 2, pcol % 2
    rows, nb = panel_ref.shape
    unit = rows // 8
    pieces = [(0, 2 * unit), (2 * unit, 2 * unit), (4 * unit, 2 * unit)]
    pieces += [(6 * unit, unit), (7 * unit, unit)]
    late = (3, 4)
    late_start = pieces[late[0]][0]
    late_span = pl.ds(late_start, rows - late_start)
    peer_pieces = [(0, 2 * unit), (2 * unit, 2 * unit), (4 * unit, unit)]
    peer_pieces += [(5 * unit, unit), (6 * unit, 2 * unit)]
    chunk = 2 * unit
    row_count, columns = slab_ref.shape
    half = columns // 2
    first_row = prow * row_count
    partner = {"prow": x * 2 + 1 - core}
    peer = {"pcol": z * 2 + 1 - y}
    left = {"pcol": (z - 1) * 2 + y}
    right = {"pcol": (z + 1) * 2 + y}
    has_left, has_right = z > 0, z < n_z - 1
    others = [{"prow": lax.rem(x + o, n_x) * 2 + core} for o in range(1, n_x)]

    barrier = pltpu.get_barrier_semaphore()
    for exists, device in ((has_left, left), (has_right, right)):
        @pl.when(exists)
        def _():
            pl.semaphore_signal(barrier, inc=1, device_id=device, device_id_type=MESH)
    fixed = [peer] + others + [partner]
    for device in fixed:
        pl.semaphore_signal(barrier, inc=1, device_id=device, device_id_type=MESH)

    panel_load = pltpu.make_async_copy(panel_ref, raw.at[z], load_sem.at[0])
    slab_load = pltpu.make_async_copy(slab_ref, slab, load_sem.at[1])
    upper_load = pltpu.make_async_copy(inv_upper_ref, inv_upper, load_sem.at[2])
    lower_load = pltpu.make_async_copy(inv_lower_ref, inv_lower, load_sem.at[3])
    pivot_load = pltpu.make_async_copy(pivots_ref, pivots, load_sem.at[4])
    pivot_row_load = pltpu.make_async_copy(pivot_row_ref, pivot_row, load_sem.at[5])
    for load in (panel_load, pivot_load, slab_load, pivot_row_load, upper_load, lower_load):
        load.start()

    def remote(source, target, send_sem, recv_sem, device):
        return pltpu.make_async_remote_copy(
            src_ref=source, dst_ref=target, send_sem=send_sem, recv_sem=recv_sem,
            device_id=device, device_id_type=MESH,
        )

    def span_of(start, count):
        return pl.ds(pl.multiple_of(start, 8), count)

    def block_at(direction, distance):
        return z - distance if direction == 0 else z + distance

    def receives(direction, distance):
        block = block_at(direction, distance)
        return block >= 0 if direction == 0 else block < n_z

    def sends(direction, distance):
        exists = has_right if direction == 0 else has_left
        return exists & receives(direction, distance)

    def guest_of(direction):
        return z == n_z - 1 if direction == 0 else z == 0

    def host_of(direction):
        return z == n_z - 2 if direction == 0 else z == 1

    def comes(direction, distance, g):
        exists = receives(direction, distance)
        if g in late:
            exists &= ~(guest_of(direction) & (distance == 1))
        return exists

    def goes(direction, g):
        exists = sends(direction, 0)
        if g in late:
            exists &= ~host_of(direction)
        return exists

    def link(direction, distance, g):
        block = block_at(direction, distance)
        spot = raw.at[block, pl.ds(*pieces[g])]
        return remote(
            spot, spot, link_send.at[direction * n_z + distance],
            link_recv.at[block * len(pieces) + g], right if direction == 0 else left,
        )

    def peer_copy(i):
        span = pl.ds(*peer_pieces[i])
        return remote(
            raw.at[z, span], raw_peer.at[span], peer_send.at[i], peer_recv.at[i], peer
        )

    panel_load.wait()
    n_peers = len(fixed) + has_left.astype(jnp.int32) + has_right.astype(jnp.int32)
    pl.semaphore_wait(barrier, n_peers)
    for g in range(len(pieces)):
        for direction in (0, 1):
            @pl.when(goes(direction, g))
            def _():
                link(direction, 0, g).start()
    for i in range(3):
        peer_copy(i).start()

    pivot_load.wait()
    slab_load.wait()

    def pick(k, carry):
        local = pivots[k] - first_row
        inside = (local >= 0) & (local < row_count)
        row = slab[pl.ds(jnp.where(inside, local, 0), 1), :]
        row = jnp.where(inside, row, 0.0)
        picked[0, pl.ds(k, 1), :] = row[:, :half]
        picked[1, pl.ds(k, 1), :] = row[:, half:]
        return carry

    lax.fori_loop(0, nb, pick, 0, unroll=8)

    pick_copy = remote(picked.at[1 - core], partner_part, pick_send, pick_recv, partner)
    pick_copy.start()
    pivot_row_load.wait()
    upper_load.wait()
    lower_load.wait()
    inv_split[0], inv_split[1] = split(inv_upper[...])
    pick_copy.wait()
    chip_sum[...] = picked[core] + partner_part[...]
    x_copies = [
        remote(chip_sum, from_x.at[i], x_send.at[i], x_recv.at[i], device)
        for i, device in enumerate(others)
    ]
    for copy in x_copies:
        copy.start()

    def pivot_hits(start, count):
        ids = first_row + start + lax.broadcasted_iota(jnp.int32, (count, nb), 0)
        return jnp.where(ids == pivot_row[...], 1.0, 0.0)

    def is_pivot(hits):
        return jnp.max(hits, axis=1, keepdims=True) > 0.0

    def solve(rows_in, hits):
        high, low = split(rows_in)
        solved = dot_split(high, low, inv_split[0], inv_split[1])
        return split(jnp.where(is_pivot(hits), -hits, solved))

    def clear(i, carry):
        start = i * 2 * chunk
        span = span_of(start, 2 * chunk)
        slab[span, :] = jnp.where(
            is_pivot(pivot_hits(start, 2 * chunk)), 0.0, slab[span, :]
        )
        return carry

    lax.fori_loop(0, row_count // (2 * chunk), clear, 0)

    def solve_rows(block, start, count):
        span = span_of(start, count)
        hits = pivot_hits((block * 2 + y) * rows + start, count)
        high, low = solve(raw[block, span, :], hits)
        lower[0, block, span, :] = high
        lower[1, block, span, :] = low

    def prepare(distance, g):
        for direction in (0, 1):
            arrives = comes(direction, distance, g)

            @pl.when(arrives)
            def _():
                link(direction, distance, g).wait_recv()

            @pl.when(arrives & sends(direction, distance))
            def _():
                link(direction, distance, g).start()

            @pl.when(arrives)
            def _():
                solve_rows(block_at(direction, distance), *pieces[g])

    for g in range(early[0]):
        prepare(1, g)

    for copy in x_copies:
        copy.wait()
    summed = chip_sum[...]
    for o in range(1, n_x):
        summed = summed + from_x[o - 1]
    total[...] = summed
    halves[core] = dot(inv_lower[...], total[...])
    to_peer = remote(
        halves.at[core], halves.at[2 + core], half_send.at[0], half_recv.at[0], peer
    )
    to_partner = remote(
        halves.at[core], halves.at[core], half_send.at[1], half_recv.at[1], partner
    )
    to_peer.start()
    to_partner.start()
    peer_copy(3).start()

    def solve_own(g, carry):
        solve_rows(z, g * chunk, chunk)
        return carry

    lax.fori_loop(0, rows // chunk, solve_own, 0)
    for g in range(early[0], early[1]):
        prepare(1, g)

    to_peer.wait()
    onward = remote(
        halves.at[2 + core], halves.at[2 + core], half_send.at[2], half_recv.at[2], partner
    )
    onward.start()
    to_partner.wait()

    def split_upper(i):
        span = slice(i * half, (i + 1) * half)
        upper[0, :, span], upper[1, :, span] = split(halves[i])

    split_upper(0)
    split_upper(1)
    onward.wait()
    split_upper(2)
    split_upper(3)

    def guest_copy(direction):
        return remote(
            halves.at[0:2], guest.at[direction], guest_send.at[direction],
            guest_recv.at[direction], left if direction == 0 else right,
        )

    def direct_copy(direction):
        return remote(
            direct.at[direction], direct_landed, direct_send.at[direction],
            direct_recv, right if direction == 0 else left,
        )

    for direction in (0, 1):
        @pl.when(guest_of(direction))
        def _():
            guest_copy(direction).start()

    def product_copy(direction, distance, g):
        block = block_at(direction, distance)
        span = pl.ds(*pieces[g])
        return remote(
            stage.at[block, span], landed.at[block, span],
            product_send.at[block], product_recv.at[block * len(pieces) + g], peer,
        )

    def subtract(block, side, start, count, product):
        span = span_of((block * 2 + side) * rows + start, count)
        slab[span, :] = slab[span, :] - product

    def multiply(distance, g):
        start, count = pieces[g]
        span = pl.ds(start, count)
        for direction in (0, 1):
            @pl.when(comes(direction, distance, g))
            def _():
                block = block_at(direction, distance)
                products = dot_split(
                    lower[0, block, span, :], lower[1, block, span, :],
                    upper[0], upper[1],
                )
                stage[block, span, :] = products[:, columns:]
                product_copy(direction, distance, g).start()
                subtract(block, y, start, count, products[:, :columns])

    def take(distance, g):
        start, count = pieces[g]
        for direction in (0, 1):
            @pl.when(comes(direction, distance, g))
            def _():
                block = block_at(direction, distance)
                product_copy(direction, distance, g).wait_recv()
                subtract(
                    block, 1 - y, start, count, landed[block, pl.ds(start, count), :]
                )

    def multiply_own(i, carry):
        span = span_of(i * chunk, chunk)
        product = dot_split(
            lower[0, z, span, :], lower[1, z, span, :],
            upper[0, :, :columns], upper[1, :, :columns],
        )
        subtract(z, y, i * chunk, chunk, product)
        return carry

    def solve_peer(start, count):
        hits = pivot_hits((z * 2 + 1 - y) * rows + start, count)
        return solve(raw_peer[pl.ds(start, count), :], hits)

    def multiply_peer(i):
        for c in ((0,), (1,), (2, 3), (4,))[i]:
            peer_copy(c).wait_recv()
        high, low = solve_peer(i * chunk, chunk)
        product = dot_split(high, low, upper[0, :, :columns], upper[1, :, :columns])
        subtract(z, 1 - y, i * chunk, chunk, product)

    def serve():
        for direction in (0, 1):
            @pl.when(host_of(direction))
            def _():
                guest_copy(direction).wait_recv()
                for i in (0, 1):
                    span = slice(i * half, (i + 1) * half)
                    guest_split[0, :, span], guest_split[1, :, span] = split(
                        guest[direction, i]
                    )
                high, low = solve_peer(late_start, rows - late_start)
                direct[direction] = dot_split(
                    jnp.concatenate([lower[0, z, late_span, :], high], axis=0),
                    jnp.concatenate([lower[1, z, late_span, :], low], axis=0),
                    guest_split[0], guest_split[1],
                )
                direct_copy(direction).start()

    for g in range(early[1]):
        multiply(1, g)
    peer_copy(4).start()
    for g in range(early[1], len(pieces)):
        prepare(1, g)
        multiply(1, g)
        lax.fori_loop(2 * (g - early[1]), 2 * (g - early[1]) + 2, multiply_own, 0)

    def step(distance, final_step):
        for g in range(len(pieces)):
            prepare(distance, g)
            multiply(distance, g)
            if isinstance(distance, int) and not final_step and g < 4:
                multiply_peer(g)
            take(distance - 1, g)
            if final_step and g >= 2:
                take(distance, g - 2)

    if n_z <= 3:
        for i in range(4):
            multiply_peer(i)
    if n_z > 3:
        step(2, False)
        lax.fori_loop(3, n_z - 1, lambda d, c: (step(d, False), c)[1], 0)
    serve()
    if n_z > 2:
        step(n_z - 1, True)

    def settle_products(direction, distance):
        block = block_at(direction, distance)

        def wait(count):
            span = pl.ds(0, count)
            remote(
                stage.at[block, span], landed.at[block, span],
                product_send.at[block], product_recv.at[0], peer,
            ).wait_send()

        whole = receives(direction, distance)
        short = guest_of(direction) & (distance == 1)
        pl.when(whole & ~short)(lambda: wait(rows))
        pl.when(whole & short)(lambda: wait(late_start))

    def settle_links(direction, distance):
        block = block_at(direction, distance)

        def wait(count):
            spot = raw.at[block, pl.ds(0, count)]
            remote(
                spot, spot, link_send.at[direction * n_z + distance], link_recv.at[0],
                right if direction == 0 else left,
            ).wait_send()

        whole = sends(direction, distance)
        short = host_of(direction) & (distance == 0)
        pl.when(whole & ~short)(lambda: wait(rows))
        pl.when(whole & short)(lambda: wait(late_start))

    def settle(distance, carry):
        for direction in (0, 1):
            settle_links(direction, distance)
        return carry

    lax.fori_loop(0, n_z - 1, settle, 0)
    for i in range(len(peer_pieces)):
        peer_copy(i).wait_send()
    for direction in (0, 1):
        @pl.when(guest_of(direction))
        def _():
            guest_copy(direction).wait_send()
    for g in range(3 if n_z > 2 else 0, len(pieces)):
        take(n_z - 1, g)

    def settle_late(distance, carry):
        for direction in (0, 1):
            settle_products(direction, distance)
        return carry

    lax.fori_loop(1, n_z, settle_late, 0)
    for direction in (0, 1):
        @pl.when(host_of(direction))
        def _():
            direct_copy(direction).wait_send()

        @pl.when(guest_of(direction))
        def _():
            direct_copy(direction).wait_recv()
            count = rows - late_start
            block = block_at(direction, 1)
            subtract(block, y, late_start, count, direct_landed[:count])
            subtract(block, 1 - y, late_start, count, direct_landed[count:])


def solution(mesh):
    n_prow, n_pcol = mesh.shape["prow"], mesh.shape["pcol"]
    n_x, n_z, n_pieces, early = n_prow // 2, n_pcol // 2, 5, (1, 3)

    def local(slab, panel, pivots, inv_lower, inv_upper):
        (row_count, columns), (rows, nb) = slab.shape, panel.shape
        half = columns // 2
        pair = rows // 2
        hbm = pl.BlockSpec(memory_space=pltpu.HBM)
        dma = pltpu.SemaphoreType.DMA
        flops = 2 * row_count * nb * (nb + columns)
        return pl.pallas_call(
            functools.partial(kernel, n_x, n_z, early),
            out_shape=pltpu.VMEM(slab.shape, slab.dtype),
            in_specs=[
                hbm,
                hbm,
                hbm,
                hbm,
                hbm,
                hbm,
            ],
            out_specs=pl.BlockSpec(memory_space=pltpu.VMEM),
            scratch_shapes=[
                pltpu.VMEM((n_z, rows, nb), F32),
                pltpu.VMEM((rows, nb), F32),
                pltpu.VMEM((2, n_z, rows, nb), BF16),
                pltpu.VMEM((n_z, rows, columns), F32),
                pltpu.VMEM((n_z, rows, columns), F32),
                pltpu.VMEM((nb, nb), F32),
                pltpu.VMEM((nb, nb), F32),
                pltpu.VMEM((2, nb, nb), BF16),
                pltpu.VMEM((2, nb, half), F32),
                pltpu.VMEM((nb, half), F32),
                pltpu.VMEM((nb, half), F32),
                pltpu.VMEM((max(n_x - 1, 1), nb, half), F32),
                pltpu.VMEM((nb, half), F32),
                pltpu.VMEM((4, nb, half), F32),
                pltpu.VMEM((2, nb, 2 * columns), BF16),
                pltpu.SMEM((nb,), jnp.int32),
                pltpu.VMEM((1, nb), jnp.int32),
                pltpu.VMEM((2, 2, nb, half), F32),
                pltpu.VMEM((2, nb, columns), BF16),
                pltpu.VMEM((2, pair, columns), F32),
                pltpu.VMEM((pair, columns), F32),
                dma((6,)),
                dma((2 * n_z,)),
                dma((n_pieces * n_z,)),
                dma((n_z,)),
                dma((n_pieces * n_z,)),
                dma,
                dma,
                dma((max(n_x - 1, 1),)),
                dma((max(n_x - 1, 1),)),
                dma((3,)),
                dma((3,)),
                dma((5,)),
                dma((5,)),
                dma((2,)),
                dma((2,)),
                dma((2,)),
                dma,
            ],
            compiler_params=pltpu.CompilerParams(
                collective_id=0, has_side_effects=True, vmem_limit_bytes=32 * 2**20
            ),
            cost_estimate=pl.CostEstimate(
                flops=flops, bytes_accessed=8 * slab.size, transcendentals=0
            ),
        )(
            *(
                pltpu.with_memory_space_constraint(a, pltpu.HBM)
                for a in (slab, panel, pivots, pivots.reshape(1, nb), inv_lower, inv_upper)
            )
        )

    return jax.shard_map(
        local,
        mesh=mesh,
        in_specs=(P("prow", "pcol"), P(("prow", "pcol"), None), P(), P(), P()),
        out_specs=P("prow", "pcol"),
        check_vma=False,
    )
```

```python
import functools

import jax
import jax.numpy as jnp
from jax import lax
from jax.experimental import pallas as pl
from jax.experimental.pallas import tpu as pltpu
from jax.sharding import PartitionSpec as P

MESH = pl.DeviceIdType.MESH
HIGHEST = lax.Precision.HIGHEST
F32 = jnp.float32
BF16 = jnp.bfloat16


def dot(a, b):
    return jnp.dot(a, b, precision=HIGHEST, preferred_element_type=F32)


def split(a):
    high = a.astype(BF16)
    return high, (a - high.astype(F32)).astype(BF16)


def dot_split(a_high, a_low, b_high, b_low):
    rows = a_high.shape[0]
    both = jnp.dot(
        jnp.concatenate([a_high, a_low], axis=0), b_high, preferred_element_type=F32
    )
    cross = jnp.dot(a_high, b_low, preferred_element_type=F32)
    return both[:rows] + (both[rows:] + cross)


def kernel(
    n_x, n_z, early,
    slab_ref, panel_ref, pivots_ref, pivot_row_ref, inv_lower_ref, inv_upper_ref,
    out_ref,
    raw, raw_peer, lower, stage, landed, inv_lower, inv_upper, inv_split,
    picked, partner_part, chip_sum, from_x, total, halves, upper, pivots, pivot_row,
    guest, guest_split, direct, direct_landed,
    load_sem, link_send, link_recv, product_send, product_recv,
    pick_send, pick_recv, x_send, x_recv, half_send, half_recv, peer_send, peer_recv,
    guest_send, guest_recv, direct_send, direct_recv,
):
    slab = out_ref
    prow = lax.axis_index("prow")
    pcol = lax.axis_index("pcol")
    x, core = prow // 2, prow % 2
    z, y = pcol // 2, pcol % 2
    rows, nb = panel_ref.shape
    unit = rows // 8
    pieces = [(0, 2 * unit), (2 * unit, 2 * unit), (4 * unit, 2 * unit)]
    pieces += [(6 * unit, unit), (7 * unit, unit)]
    late = (3, 4)
    late_start = pieces[late[0]][0]
    late_span = pl.ds(late_start, rows - late_start)
    peer_pieces = [(0, 2 * unit), (2 * unit, 2 * unit), (4 * unit, unit)]
    peer_pieces += [(5 * unit, unit), (6 * unit, 2 * unit)]
    chunk = 2 * unit
    row_count, columns = slab_ref.shape
    half = columns // 2
    first_row = prow * row_count
    partner = {"prow": x * 2 + 1 - core}
    peer = {"pcol": z * 2 + 1 - y}
    left = {"pcol": (z - 1) * 2 + y}
    right = {"pcol": (z + 1) * 2 + y}
    has_left, has_right = z > 0, z < n_z - 1
    others = [{"prow": lax.rem(x + o, n_x) * 2 + core} for o in range(1, n_x)]

    barrier = pltpu.get_barrier_semaphore()
    for exists, device in ((has_left, left), (has_right, right)):
        @pl.when(exists)
        def _():
            pl.semaphore_signal(barrier, inc=1, device_id=device, device_id_type=MESH)
    fixed = [peer] + others + [partner]
    for device in fixed:
        pl.semaphore_signal(barrier, inc=1, device_id=device, device_id_type=MESH)

    panel_load = pltpu.make_async_copy(panel_ref, raw.at[z], load_sem.at[0])
    slab_load = pltpu.make_async_copy(slab_ref, slab, load_sem.at[1])
    upper_load = pltpu.make_async_copy(inv_upper_ref, inv_upper, load_sem.at[2])
    lower_load = pltpu.make_async_copy(inv_lower_ref, inv_lower, load_sem.at[3])
    pivot_load = pltpu.make_async_copy(pivots_ref, pivots, load_sem.at[4])
    pivot_row_load = pltpu.make_async_copy(pivot_row_ref, pivot_row, load_sem.at[5])
    for load in (panel_load, pivot_load, slab_load, pivot_row_load, upper_load, lower_load):
        load.start()

    def remote(source, target, send_sem, recv_sem, device):
        return pltpu.make_async_remote_copy(
            src_ref=source, dst_ref=target, send_sem=send_sem, recv_sem=recv_sem,
            device_id=device, device_id_type=MESH,
        )

    def span_of(start, count):
        return pl.ds(pl.multiple_of(start, 8), count)

    def block_at(direction, distance):
        return z - distance if direction == 0 else z + distance

    def receives(direction, distance):
        block = block_at(direction, distance)
        return block >= 0 if direction == 0 else block < n_z

    def sends(direction, distance):
        exists = has_right if direction == 0 else has_left
        return exists & receives(direction, distance)

    def guest_of(direction):
        return z == n_z - 1 if direction == 0 else z == 0

    def host_of(direction):
        return z == n_z - 2 if direction == 0 else z == 1

    def comes(direction, distance, g):
        exists = receives(direction, distance)
        if g in late:
            exists &= ~(guest_of(direction) & (distance == 1))
        return exists

    def goes(direction, g):
        exists = sends(direction, 0)
        if g in late:
            exists &= ~host_of(direction)
        return exists

    def link(direction, distance, g):
        block = block_at(direction, distance)
        spot = raw.at[block, pl.ds(*pieces[g])]
        return remote(
            spot, spot, link_send.at[direction * n_z + distance],
            link_recv.at[(block - direction) * len(pieces) + g],
            right if direction == 0 else left,
        )

    def peer_copy(i):
        span = pl.ds(*peer_pieces[i])
        return remote(
            raw.at[z, span], raw_peer.at[span], peer_send, peer_recv.at[i], peer
        )

    panel_load.wait()
    n_peers = len(fixed) + has_left.astype(jnp.int32) + has_right.astype(jnp.int32)
    pl.semaphore_wait(barrier, n_peers)
    def start_links():
        for loaded in (True, False):
            for direction in (0, 1):
                near = (2 * z < n_z) if direction == 1 else (2 * z >= n_z)
                for g in range(len(pieces)):
                    @pl.when(goes(direction, g) & (near if loaded else ~near))
                    def _():
                        link(direction, 0, g).start()

    pl.when(core == 0)(start_links)
    for i in range(3):
        peer_copy(i).start()

    pivot_load.wait()
    slab_load.wait()
    pl.when(core != 0)(start_links)

    def pick(k, carry):
        local = pivots[k] - first_row
        inside = (local >= 0) & (local < row_count)
        row = slab[pl.ds(jnp.where(inside, local, 0), 1), :]
        row = jnp.where(inside, row, 0.0)
        picked[0, pl.ds(k, 1), :] = row[:, :half]
        picked[1, pl.ds(k, 1), :] = row[:, half:]
        return carry

    lax.fori_loop(0, nb, pick, 0, unroll=8)

    pick_copy = remote(picked.at[1 - core], partner_part, pick_send, pick_recv, partner)
    pick_copy.start()
    pivot_row_load.wait()
    upper_load.wait()
    lower_load.wait()
    inv_split[0], inv_split[1] = split(inv_upper[...])
    pick_copy.wait()
    chip_sum[...] = picked[core] + partner_part[...]
    x_copies = [
        remote(chip_sum, from_x.at[i], x_send.at[i], x_recv.at[i], device)
        for i, device in enumerate(others)
    ]
    for copy in x_copies:
        copy.start()

    def pivot_hits(start, count):
        ids = first_row + start + lax.broadcasted_iota(jnp.int32, (count, nb), 0)
        return jnp.where(ids == pivot_row[...], 1.0, 0.0)

    def is_pivot(hits):
        return jnp.max(hits, axis=1, keepdims=True) > 0.0

    def solve(rows_in, hits):
        high, low = split(rows_in)
        solved = dot_split(high, low, inv_split[0], inv_split[1])
        return split(jnp.where(is_pivot(hits), -hits, solved))

    def clear(i, carry):
        start = i * 2 * chunk
        span = span_of(start, 2 * chunk)
        slab[span, :] = jnp.where(
            is_pivot(pivot_hits(start, 2 * chunk)), 0.0, slab[span, :]
        )
        return carry

    lax.fori_loop(0, row_count // (2 * chunk), clear, 0)

    def solve_rows(block, start, count):
        span = span_of(start, count)
        hits = pivot_hits((block * 2 + y) * rows + start, count)
        high, low = solve(raw[block, span, :], hits)
        lower[0, block, span, :] = high
        lower[1, block, span, :] = low

    def prepare(distance, g):
        for direction in (0, 1):
            arrives = comes(direction, distance, g)

            @pl.when(arrives)
            def _():
                link(direction, distance, g).wait_recv()

            @pl.when(arrives & sends(direction, distance))
            def _():
                link(direction, distance, g).start()

            @pl.when(arrives)
            def _():
                solve_rows(block_at(direction, distance), *pieces[g])

    for g in range(early[0]):
        prepare(1, g)

    for copy in x_copies:
        copy.wait()
    summed = chip_sum[...]
    for o in range(1, n_x):
        summed = summed + from_x[o - 1]
    total[...] = summed
    halves[core] = dot(inv_lower[...], total[...])
    to_peer = remote(
        halves.at[core], halves.at[2 + core], half_send.at[0], half_recv.at[0], peer
    )
    to_partner = remote(
        halves.at[core], halves.at[core], half_send.at[1], half_recv.at[1], partner
    )
    to_peer.start()
    to_partner.start()
    peer_copy(3).start()

    def solve_own(g, carry):
        solve_rows(z, g * chunk, chunk)
        return carry

    lax.fori_loop(0, rows // chunk, solve_own, 0)
    for g in range(early[0], early[1]):
        prepare(1, g)

    to_peer.wait()
    onward = remote(
        halves.at[2 + core], halves.at[2 + core], half_send.at[2], half_recv.at[2], partner
    )
    onward.start()
    to_partner.wait()

    def split_upper(i):
        span = slice(i * half, (i + 1) * half)
        upper[0, :, span], upper[1, :, span] = split(halves[i])

    split_upper(0)
    split_upper(1)
    onward.wait()
    split_upper(2)
    split_upper(3)

    def guest_copy(direction):
        return remote(
            halves.at[0:2], guest.at[direction], guest_send.at[direction],
            guest_recv.at[direction], left if direction == 0 else right,
        )

    def direct_copy(direction):
        return remote(
            direct.at[direction], direct_landed, direct_send.at[direction],
            direct_recv, right if direction == 0 else left,
        )

    for direction in (0, 1):
        @pl.when(guest_of(direction))
        def _():
            guest_copy(direction).start()

    def product_copy(direction, distance, g):
        block = block_at(direction, distance)
        span = pl.ds(*pieces[g])
        return remote(
            stage.at[block, span], landed.at[block, span],
            product_send.at[block - direction],
            product_recv.at[(block - direction) * len(pieces) + g], peer,
        )

    def subtract(block, side, start, count, product):
        span = span_of((block * 2 + side) * rows + start, count)
        slab[span, :] = slab[span, :] - product

    def multiply(distance, g):
        start, count = pieces[g]
        span = pl.ds(start, count)
        for direction in (0, 1):
            @pl.when(comes(direction, distance, g))
            def _():
                block = block_at(direction, distance)
                products = dot_split(
                    lower[0, block, span, :], lower[1, block, span, :],
                    upper[0], upper[1],
                )
                stage[block, span, :] = products[:, columns:]
                product_copy(direction, distance, g).start()
                subtract(block, y, start, count, products[:, :columns])

    def take(distance, g):
        start, count = pieces[g]
        for direction in (0, 1):
            @pl.when(comes(direction, distance, g))
            def _():
                block = block_at(direction, distance)
                product_copy(direction, distance, g).wait_recv()
                subtract(
                    block, 1 - y, start, count, landed[block, pl.ds(start, count), :]
                )

    def multiply_own(i, carry):
        span = span_of(i * chunk, chunk)
        product = dot_split(
            lower[0, z, span, :], lower[1, z, span, :],
            upper[0, :, :columns], upper[1, :, :columns],
        )
        subtract(z, y, i * chunk, chunk, product)
        return carry

    def solve_peer(start, count):
        hits = pivot_hits((z * 2 + 1 - y) * rows + start, count)
        return solve(raw_peer[pl.ds(start, count), :], hits)

    def multiply_peer(i):
        for c in ((0,), (1,), (2, 3), (4,))[i]:
            peer_copy(c).wait_recv()
        high, low = solve_peer(i * chunk, chunk)
        product = dot_split(high, low, upper[0, :, :columns], upper[1, :, :columns])
        subtract(z, 1 - y, i * chunk, chunk, product)

    def serve():
        for direction in (0, 1):
            @pl.when(host_of(direction))
            def _():
                guest_copy(direction).wait_recv()
                for i in (0, 1):
                    span = slice(i * half, (i + 1) * half)
                    guest_split[0, :, span], guest_split[1, :, span] = split(
                        guest[direction, i]
                    )
                high, low = solve_peer(late_start, rows - late_start)
                direct[direction] = dot_split(
                    jnp.concatenate([lower[0, z, late_span, :], high], axis=0),
                    jnp.concatenate([lower[1, z, late_span, :], low], axis=0),
                    guest_split[0], guest_split[1],
                )
                direct_copy(direction).start()

    for g in range(early[1]):
        multiply(1, g)
    peer_copy(4).start()
    for g in range(early[1], len(pieces)):
        prepare(1, g)
        multiply(1, g)
        lax.fori_loop(2 * (g - early[1]), 2 * (g - early[1]) + 2, multiply_own, 0)

    def step(distance, final_step):
        for g in range(len(pieces)):
            prepare(distance, g)
            multiply(distance, g)
            if isinstance(distance, int) and not final_step and g < 4:
                multiply_peer(g)
            take(distance - 1, g)
            if final_step and g >= 2:
                take(distance, g - 2)

    if n_z <= 3:
        for i in range(4):
            multiply_peer(i)
    if n_z > 3:
        step(2, False)
        lax.fori_loop(3, n_z - 1, lambda d, c: (step(d, False), c)[1], 0)
    serve()
    if n_z > 2:
        step(n_z - 1, True)

    def settle_products(direction, distance):
        block = block_at(direction, distance)

        def wait(count):
            span = pl.ds(0, count)
            remote(
                stage.at[block, span], landed.at[block, span],
                product_send.at[block - direction], product_recv.at[0], peer,
            ).wait_send()

        whole = receives(direction, distance)
        short = guest_of(direction) & (distance == 1)
        pl.when(whole & ~short)(lambda: wait(rows))
        pl.when(whole & short)(lambda: wait(late_start))

    def settle_links(direction, distance):
        block = block_at(direction, distance)

        def wait(count):
            spot = raw.at[block, pl.ds(0, count)]
            remote(
                spot, spot, link_send.at[direction * n_z + distance], link_recv.at[0],
                right if direction == 0 else left,
            ).wait_send()

        whole = sends(direction, distance)
        short = host_of(direction) & (distance == 0)
        pl.when(whole & ~short)(lambda: wait(rows))
        pl.when(whole & short)(lambda: wait(late_start))

    def settle(distance, carry):
        for direction in (0, 1):
            settle_links(direction, distance)
        return carry

    lax.fori_loop(0, n_z - 1, settle, 0)
    remote(raw.at[z], raw_peer, peer_send, peer_recv.at[0], peer).wait_send()
    for direction in (0, 1):
        @pl.when(guest_of(direction))
        def _():
            guest_copy(direction).wait_send()
    for g in range(3 if n_z > 2 else 0, len(pieces)):
        take(n_z - 1, g)

    def settle_late(distance, carry):
        for direction in (0, 1):
            settle_products(direction, distance)
        return carry

    lax.fori_loop(1, n_z, settle_late, 0)
    for direction in (0, 1):
        @pl.when(host_of(direction))
        def _():
            direct_copy(direction).wait_send()

        @pl.when(guest_of(direction))
        def _():
            direct_copy(direction).wait_recv()
            count = rows - late_start
            block = block_at(direction, 1)
            subtract(block, y, late_start, count, direct_landed[:count])
            subtract(block, 1 - y, late_start, count, direct_landed[count:])


def solution(mesh):
    n_prow, n_pcol = mesh.shape["prow"], mesh.shape["pcol"]
    n_x, n_z, n_pieces, early = n_prow // 2, n_pcol // 2, 5, (1, 3)

    def local(slab, panel, pivots, inv_lower, inv_upper):
        (row_count, columns), (rows, nb) = slab.shape, panel.shape
        half = columns // 2
        pair = rows // 2
        hbm = pl.BlockSpec(memory_space=pltpu.HBM)
        dma = pltpu.SemaphoreType.DMA
        flops = 2 * row_count * nb * (nb + columns)
        return pl.pallas_call(
            functools.partial(kernel, n_x, n_z, early),
            out_shape=pltpu.VMEM(slab.shape, slab.dtype),
            in_specs=[
                hbm,
                hbm,
                hbm,
                hbm,
                hbm,
                hbm,
            ],
            out_specs=pl.BlockSpec(memory_space=pltpu.VMEM),
            scratch_shapes=[
                pltpu.VMEM((n_z, rows, nb), F32),
                pltpu.VMEM((rows, nb), F32),
                pltpu.VMEM((2, n_z, rows, nb), BF16),
                pltpu.VMEM((n_z, rows, columns), F32),
                pltpu.VMEM((n_z, rows, columns), F32),
                pltpu.VMEM((nb, nb), F32),
                pltpu.VMEM((nb, nb), F32),
                pltpu.VMEM((2, nb, nb), BF16),
                pltpu.VMEM((2, nb, half), F32),
                pltpu.VMEM((nb, half), F32),
                pltpu.VMEM((nb, half), F32),
                pltpu.VMEM((max(n_x - 1, 1), nb, half), F32),
                pltpu.VMEM((nb, half), F32),
                pltpu.VMEM((4, nb, half), F32),
                pltpu.VMEM((2, nb, 2 * columns), BF16),
                pltpu.SMEM((nb,), jnp.int32),
                pltpu.VMEM((1, nb), jnp.int32),
                pltpu.VMEM((2, 2, nb, half), F32),
                pltpu.VMEM((2, nb, columns), BF16),
                pltpu.VMEM((2, pair, columns), F32),
                pltpu.VMEM((pair, columns), F32),
                dma((6,)),
                dma((2 * n_z,)),
                dma((n_pieces * (n_z - 1),)),
                dma((n_z - 1,)),
                dma((n_pieces * (n_z - 1),)),
                dma,
                dma,
                dma((max(n_x - 1, 1),)),
                dma((max(n_x - 1, 1),)),
                dma((3,)),
                dma((3,)),
                dma,
                dma((5,)),
                dma((2,)),
                dma((2,)),
                dma((2,)),
                dma,
            ],
            compiler_params=pltpu.CompilerParams(
                collective_id=0, has_side_effects=True, vmem_limit_bytes=32 * 2**20
            ),
            cost_estimate=pl.CostEstimate(
                flops=flops, bytes_accessed=8 * slab.size, transcendentals=0
            ),
        )(
            *(
                pltpu.with_memory_space_constraint(a, pltpu.HBM)
                for a in (slab, panel, pivots, pivots.reshape(1, nb), inv_lower, inv_upper)
            )
        )

    return jax.shard_map(
        local,
        mesh=mesh,
        in_specs=(P("prow", "pcol"), P(("prow", "pcol"), None), P(), P(), P()),
        out_specs=P("prow", "pcol"),
        check_vma=False,
    )
```

```python
import functools

import jax
import jax.numpy as jnp
from jax import lax
from jax.experimental import pallas as pl
from jax.experimental.pallas import tpu as pltpu
from jax.sharding import PartitionSpec as P

MESH = pl.DeviceIdType.MESH
HIGHEST = lax.Precision.HIGHEST
F32 = jnp.float32
BF16 = jnp.bfloat16


def dot(a, b):
    return jnp.dot(a, b, precision=HIGHEST, preferred_element_type=F32)


def split(a):
    high = a.astype(BF16)
    return high, (a - high.astype(F32)).astype(BF16)


def dot_split(a_high, a_low, b_high, b_low):
    rows = a_high.shape[0]
    both = jnp.dot(
        jnp.concatenate([a_high, a_low], axis=0), b_high, preferred_element_type=F32
    )
    cross = jnp.dot(a_high, b_low, preferred_element_type=F32)
    return both[:rows] + (both[rows:] + cross)


def kernel(
    n_x, n_z, early,
    slab_ref, panel_ref, pivots_ref, pivot_row_ref, inv_lower_ref, inv_upper_ref,
    out_ref,
    raw, raw_peer, lower, stage, landed, inv_lower, inv_upper, inv_split,
    picked, partner_part, chip_sum, from_x, total, halves, upper, pivots, pivot_row,
    guest, guest_split, direct, direct_landed,
    load_sem, link_send, link_recv, product_send, product_recv,
    pick_send, pick_recv, x_send, x_recv, half_send, half_recv, peer_send, peer_recv,
    detour, guest_send, guest_recv, direct_send, direct_recv, detour_send, detour_recv,
):
    slab = out_ref
    prow = lax.axis_index("prow")
    pcol = lax.axis_index("pcol")
    x, core = prow // 2, prow % 2
    z, y = pcol // 2, pcol % 2
    rows, nb = panel_ref.shape
    unit = rows // 8
    step_rows = rows // 16
    pieces, edge = [], 0
    for size in (4, 4, 3, 3, 2):
        pieces.append((edge, size * step_rows))
        edge += size * step_rows
    groups = [(0, pieces[3][0]), (pieces[3][0], rows - pieces[3][0])]
    late = (3, 4)
    late_start = pieces[late[0]][0]
    late_span = pl.ds(late_start, rows - late_start)
    peer_pieces = [(0, 2 * unit), (2 * unit, 2 * unit), (4 * unit, unit)]
    peer_pieces += [(5 * unit, unit), (6 * unit, 2 * unit)]
    chunk = 2 * unit
    row_count, columns = slab_ref.shape
    half = columns // 2
    first_row = prow * row_count
    partner = {"prow": x * 2 + 1 - core}
    peer = {"pcol": z * 2 + 1 - y}
    left = {"pcol": (z - 1) * 2 + y}
    right = {"pcol": (z + 1) * 2 + y}
    has_left, has_right = z > 0, z < n_z - 1
    others = [{"prow": lax.rem(x + o, n_x) * 2 + core} for o in range(1, n_x)]

    barrier = pltpu.get_barrier_semaphore()
    for exists, device in ((has_left, left), (has_right, right)):
        @pl.when(exists)
        def _():
            pl.semaphore_signal(barrier, inc=1, device_id=device, device_id_type=MESH)
    fixed = [peer] + others + [partner]
    for device in fixed:
        pl.semaphore_signal(barrier, inc=1, device_id=device, device_id_type=MESH)

    panel_load = pltpu.make_async_copy(panel_ref, raw.at[z], load_sem.at[0])
    slab_load = pltpu.make_async_copy(slab_ref, slab, load_sem.at[1])
    upper_load = pltpu.make_async_copy(inv_upper_ref, inv_upper, load_sem.at[2])
    lower_load = pltpu.make_async_copy(inv_lower_ref, inv_lower, load_sem.at[3])
    pivot_load = pltpu.make_async_copy(pivots_ref, pivots, load_sem.at[4])
    pivot_row_load = pltpu.make_async_copy(pivot_row_ref, pivot_row, load_sem.at[5])
    for load in (panel_load, pivot_load, slab_load, pivot_row_load, upper_load, lower_load):
        load.start()

    def remote(source, target, send_sem, recv_sem, device):
        return pltpu.make_async_remote_copy(
            src_ref=source, dst_ref=target, send_sem=send_sem, recv_sem=recv_sem,
            device_id=device, device_id_type=MESH,
        )

    def span_of(start, count):
        return pl.ds(pl.multiple_of(start, 8), count)

    def block_at(direction, distance):
        return z - distance if direction == 0 else z + distance

    def receives(direction, distance):
        block = block_at(direction, distance)
        return block >= 0 if direction == 0 else block < n_z

    def sends(direction, distance):
        exists = has_right if direction == 0 else has_left
        return exists & receives(direction, distance)

    def guest_of(direction):
        return z == n_z - 1 if direction == 0 else z == 0

    def host_of(direction):
        return z == n_z - 2 if direction == 0 else z == 1

    def comes(direction, distance, g):
        exists = receives(direction, distance)
        if g in late:
            exists &= ~(guest_of(direction) & (distance == 1))
        return exists

    def goes(direction, g):
        exists = sends(direction, 0)
        if g in late:
            exists &= ~host_of(direction)
        return exists

    def link(direction, distance, g):
        block = block_at(direction, distance)
        spot = raw.at[block, pl.ds(*pieces[g])]
        return remote(
            spot, spot, link_send.at[direction * (n_z - 1) + distance % (n_z - 1)],
            link_recv.at[(block - direction) * len(pieces) + g],
            right if direction == 0 else left,
        )

    def peer_copy(i):
        span = pl.ds(*peer_pieces[i])
        return remote(
            raw.at[z, span], raw_peer.at[span], peer_send, peer_recv.at[i], peer
        )

    panel_load.wait()
    n_peers = len(fixed) + has_left.astype(jnp.int32) + has_right.astype(jnp.int32)
    pl.semaphore_wait(barrier, n_peers)
    for g in range(len(pieces)):
        for direction in (0, 1):
            @pl.when(goes(direction, g))
            def _():
                link(direction, 0, g).start()

    for i in range(3):
        peer_copy(i).start()

    pivot_load.wait()
    slab_load.wait()

    def pick(k, carry):
        local = pivots[k] - first_row
        inside = (local >= 0) & (local < row_count)
        row = slab[pl.ds(jnp.where(inside, local, 0), 1), :]
        row = jnp.where(inside, row, 0.0)
        picked[0, pl.ds(k, 1), :] = row[:, :half]
        picked[1, pl.ds(k, 1), :] = row[:, half:]
        return carry

    lax.fori_loop(0, nb, pick, 0, unroll=8)

    pick_copy = remote(picked.at[1 - core], partner_part, pick_send, pick_recv, partner)
    pick_copy.start()
    pivot_row_load.wait()
    upper_load.wait()
    lower_load.wait()
    inv_split[0], inv_split[1] = split(inv_upper[...])
    pick_copy.wait()
    chip_sum[...] = picked[core] + partner_part[...]
    x_copies = [
        remote(chip_sum, from_x.at[i], x_send.at[i], x_recv.at[i], device)
        for i, device in enumerate(others)
    ]
    for copy in x_copies:
        copy.start()

    def pivot_hits(start, count):
        ids = first_row + start + lax.broadcasted_iota(jnp.int32, (count, nb), 0)
        return jnp.where(ids == pivot_row[...], 1.0, 0.0)

    def is_pivot(hits):
        return jnp.max(hits, axis=1, keepdims=True) > 0.0

    def solve(rows_in, hits):
        high, low = split(rows_in)
        solved = dot_split(high, low, inv_split[0], inv_split[1])
        return split(jnp.where(is_pivot(hits), -hits, solved))

    def clear(i, carry):
        start = i * 2 * chunk
        span = span_of(start, 2 * chunk)
        slab[span, :] = jnp.where(
            is_pivot(pivot_hits(start, 2 * chunk)), 0.0, slab[span, :]
        )
        return carry

    lax.fori_loop(0, row_count // (2 * chunk), clear, 0)

    def solve_rows(block, start, count):
        span = span_of(start, count)
        hits = pivot_hits((block * 2 + y) * rows + start, count)
        high, low = solve(raw[block, span, :], hits)
        lower[0, block, span, :] = high
        lower[1, block, span, :] = low

    def prepare(distance, g):
        for direction in (0, 1):
            arrives = comes(direction, distance, g)

            @pl.when(arrives)
            def _():
                link(direction, distance, g).wait_recv()

            @pl.when(arrives & sends(direction, distance))
            def _():
                link(direction, distance, g).start()

            @pl.when(arrives)
            def _():
                solve_rows(block_at(direction, distance), *pieces[g])

    for g in range(early[0]):
        prepare(1, g)

    for copy in x_copies:
        copy.wait()
    summed = chip_sum[...]
    for o in range(1, n_x):
        summed = summed + from_x[o - 1]
    total[...] = summed
    halves[core] = dot(inv_lower[...], total[...])
    to_peer = remote(
        halves.at[core], halves.at[2 + core], half_send.at[0], half_recv.at[0], peer
    )
    to_partner = remote(
        halves.at[core], halves.at[core], half_send.at[1], half_recv.at[1], partner
    )
    to_peer.start()
    to_partner.start()
    peer_copy(3).start()

    def solve_own(g, carry):
        solve_rows(z, g * chunk, chunk)
        return carry

    lax.fori_loop(0, rows // chunk, solve_own, 0)
    for g in range(early[0], early[1]):
        prepare(1, g)

    to_peer.wait()
    onward = remote(
        halves.at[2 + core], halves.at[2 + core], half_send.at[2], half_recv.at[2], partner
    )
    onward.start()
    to_partner.wait()

    def split_upper(i):
        span = slice(i * half, (i + 1) * half)
        upper[0, :, span], upper[1, :, span] = split(halves[i])

    split_upper(0)
    split_upper(1)
    onward.wait()
    split_upper(2)
    split_upper(3)

    def guest_copy(direction):
        return remote(
            halves.at[0:2], guest.at[direction], guest_send.at[direction],
            guest_recv.at[direction], left if direction == 0 else right,
        )

    full = direct_landed.shape[0]
    kept = full - detour.shape[0]
    first = (x == 0) & (y == 0) & (n_x > 1)
    helper = (x == 1) & (y == 0)

    def direct_copy(direction, count):
        return remote(
            direct.at[direction, pl.ds(0, count)], direct_landed.at[pl.ds(0, count)],
            direct_send.at[direction], direct_recv,
            right if direction == 0 else left,
        )

    def detour_copy(leg):
        source = direct.at[1, pl.ds(kept, full - kept)] if leg == 0 else detour
        target = direct_landed.at[pl.ds(kept, full - kept)] if leg == 2 else detour
        device = ({"prow": 2 + core}, left, {"prow": core})[leg]
        return remote(source, target, detour_send, detour_recv, device)

    def of_first(direction):
        return first if direction == 1 else x < 0

    for direction in (0, 1):
        @pl.when(guest_of(direction))
        def _():
            guest_copy(direction).start()

    def product_copy(direction, distance, g):
        block = block_at(direction, distance)
        span = pl.ds(*pieces[g])
        return remote(
            stage.at[block, span], landed.at[block, span],
            product_send.at[block - direction],
            product_recv.at[(block - direction) * 2 + g // 3], peer,
        )

    def subtract(block, side, start, count, product):
        span = span_of((block * 2 + side) * rows + start, count)
        slab[span, :] = slab[span, :] - product

    def multiply(distance, g):
        start, count = pieces[g]
        span = pl.ds(start, count)
        for direction in (0, 1):
            @pl.when(comes(direction, distance, g))
            def _():
                block = block_at(direction, distance)
                products = dot_split(
                    lower[0, block, span, :], lower[1, block, span, :],
                    upper[0], upper[1],
                )
                stage[block, span, :] = products[:, columns:]
                product_copy(direction, distance, g).start()
                subtract(block, y, start, count, products[:, :columns])

    def take(distance, group):
        start, count = groups[group]
        for direction in (0, 1):
            @pl.when(comes(direction, distance, 3 * group))
            def _():
                block = block_at(direction, distance)
                landing = landed.at[block, pl.ds(start, count)]
                remote(
                    landing, landing, product_send.at[block - direction],
                    product_recv.at[(block - direction) * 2 + group], peer,
                ).wait_recv()
                subtract(
                    block, 1 - y, start, count, landed[block, pl.ds(start, count), :]
                )

    def multiply_own(i, carry):
        span = span_of(i * chunk, chunk)
        product = dot_split(
            lower[0, z, span, :], lower[1, z, span, :],
            upper[0, :, :columns], upper[1, :, :columns],
        )
        subtract(z, y, i * chunk, chunk, product)
        return carry

    def solve_peer(start, count):
        hits = pivot_hits((z * 2 + 1 - y) * rows + start, count)
        return solve(raw_peer[pl.ds(start, count), :], hits)

    def multiply_peer(i):
        for c in ((0,), (1,), (2, 3), (4,))[i]:
            peer_copy(c).wait_recv()
        high, low = solve_peer(i * chunk, chunk)
        product = dot_split(high, low, upper[0, :, :columns], upper[1, :, :columns])
        subtract(z, 1 - y, i * chunk, chunk, product)

    def serve():
        for direction in (0, 1):
            @pl.when(host_of(direction))
            def _():
                guest_copy(direction).wait_recv()
                for i in (0, 1):
                    span = slice(i * half, (i + 1) * half)
                    guest_split[0, :, span], guest_split[1, :, span] = split(
                        guest[direction, i]
                    )
                high, low = solve_peer(late_start, rows - late_start)
                direct[direction] = dot_split(
                    jnp.concatenate([lower[0, z, late_span, :], high], axis=0),
                    jnp.concatenate([lower[1, z, late_span, :], low], axis=0),
                    guest_split[0], guest_split[1],
                )
                if direction == 1:
                    @pl.when(first)
                    def _():
                        detour_copy(0).start()

                    @pl.when(helper)
                    def _():
                        detour_copy(0).wait_recv()
                        detour_copy(1).start()

    def start_direct():
        for direction in (0, 1):
            @pl.when(host_of(direction) & of_first(direction))
            def _():
                direct_copy(direction, kept).start()

            @pl.when(host_of(direction) & ~of_first(direction))
            def _():
                direct_copy(direction, full).start()

    for g in range(early[1]):
        multiply(1, g)
    peer_copy(4).start()
    for g in range(early[1], len(pieces)):
        prepare(1, g)
        multiply(1, g)
        lax.fori_loop(2 * (g - early[1]), 2 * (g - early[1]) + 2, multiply_own, 0)

    def pass_detour():
        @pl.when(guest_of(1) & helper)
        def _():
            detour_copy(1).wait_recv()
            detour_copy(2).start()

    def step(distance, final_step):
        for g in range(len(pieces)):
            prepare(distance, g)
            multiply(distance, g)
            if isinstance(distance, int) and not final_step and g < 4:
                multiply_peer(g)
            if isinstance(distance, int) and not final_step and g == 3:
                serve()
            if g in (2, 4):
                take(distance - 1, g // 4)
            if final_step and g == 3:
                pass_detour()
            if final_step and g == 4:
                take(distance, 0)

    if n_z <= 3:
        for i in range(4):
            multiply_peer(i)
    if n_z > 3:
        step(2, False)
        lax.fori_loop(3, n_z - 1, lambda d, c: (step(d, False), c)[1], 0)
    if n_z <= 3:
        serve()
    start_direct()
    if n_z > 2:
        step(n_z - 1, True)
    else:
        pass_detour()

    def settle_products(direction, distance):
        block = block_at(direction, distance)

        def wait(count):
            span = pl.ds(0, count)
            remote(
                stage.at[block, span], landed.at[block, span],
                product_send.at[block - direction], product_recv.at[0], peer,
            ).wait_send()

        whole = receives(direction, distance)
        short = guest_of(direction) & (distance == 1)
        pl.when(whole & ~short)(lambda: wait(rows))
        pl.when(whole & short)(lambda: wait(late_start))

    def settle_links(direction, distance):
        block = block_at(direction, distance)

        def wait(count):
            spot = raw.at[block, pl.ds(0, count)]
            remote(
                spot, spot, link_send.at[direction * (n_z - 1) + distance % (n_z - 1)], link_recv.at[0],
                right if direction == 0 else left,
            ).wait_send()

        whole = sends(direction, distance)
        short = host_of(direction) & (distance == 0)
        pl.when(whole & ~short)(lambda: wait(rows))
        pl.when(whole & short)(lambda: wait(late_start))

    def settle(distance, carry):
        for direction in (0, 1):
            settle_links(direction, distance)
        return carry

    lax.fori_loop(0, n_z - 1, settle, 0)
    remote(raw.at[z], raw_peer, peer_send, peer_recv.at[0], peer).wait_send()
    for direction in (0, 1):
        @pl.when(guest_of(direction))
        def _():
            guest_copy(direction).wait_send()
    for group in range(1 if n_z > 2 else 0, 2):
        take(n_z - 1, group)

    def settle_late(distance, carry):
        for direction in (0, 1):
            settle_products(direction, distance)
        return carry

    lax.fori_loop(1, n_z, settle_late, 0)
    for direction in (0, 1):
        @pl.when(host_of(direction))
        def _():
            @pl.when(of_first(direction))
            def _():
                direct_copy(direction, kept).wait_send()
                detour_copy(0).wait_send()

            @pl.when(~of_first(direction))
            def _():
                direct_copy(direction, full).wait_send()

            if direction == 1:
                @pl.when(helper)
                def _():
                    detour_copy(1).wait_send()

        @pl.when(guest_of(direction))
        def _():
            @pl.when(of_first(direction))
            def _():
                direct_copy(direction, kept).wait_recv()
                detour_copy(2).wait_recv()

            @pl.when(~of_first(direction))
            def _():
                direct_copy(direction, full).wait_recv()

            if direction == 1:
                @pl.when(helper)
                def _():
                    detour_copy(2).wait_send()

            count = rows - late_start
            block = block_at(direction, 1)
            subtract(block, y, late_start, count, direct_landed[:count])
            subtract(block, 1 - y, late_start, count, direct_landed[count:])


def solution(mesh):
    n_prow, n_pcol = mesh.shape["prow"], mesh.shape["pcol"]
    n_x, n_z, n_pieces, early = n_prow // 2, n_pcol // 2, 5, (1, 3)

    def local(slab, panel, pivots, inv_lower, inv_upper):
        (row_count, columns), (rows, nb) = slab.shape, panel.shape
        half = columns // 2
        pair = rows * 5 // 8
        hbm = pl.BlockSpec(memory_space=pltpu.HBM)
        dma = pltpu.SemaphoreType.DMA
        flops = 2 * row_count * nb * (nb + columns)
        return pl.pallas_call(
            functools.partial(kernel, n_x, n_z, early),
            out_shape=pltpu.VMEM(slab.shape, slab.dtype),
            in_specs=[
                hbm,
                hbm,
                hbm,
                hbm,
                hbm,
                hbm,
            ],
            out_specs=pl.BlockSpec(memory_space=pltpu.VMEM),
            scratch_shapes=[
                pltpu.VMEM((n_z, rows, nb), F32),
                pltpu.VMEM((rows, nb), F32),
                pltpu.VMEM((2, n_z, rows, nb), BF16),
                pltpu.VMEM((n_z, rows, columns), F32),
                pltpu.VMEM((n_z, rows, columns), F32),
                pltpu.VMEM((nb, nb), F32),
                pltpu.VMEM((nb, nb), F32),
                pltpu.VMEM((2, nb, nb), BF16),
                pltpu.VMEM((2, nb, half), F32),
                pltpu.VMEM((nb, half), F32),
                pltpu.VMEM((nb, half), F32),
                pltpu.VMEM((max(n_x - 1, 1), nb, half), F32),
                pltpu.VMEM((nb, half), F32),
                pltpu.VMEM((4, nb, half), F32),
                pltpu.VMEM((2, nb, 2 * columns), BF16),
                pltpu.SMEM((nb,), jnp.int32),
                pltpu.VMEM((1, nb), jnp.int32),
                pltpu.VMEM((2, 2, nb, half), F32),
                pltpu.VMEM((2, nb, columns), BF16),
                pltpu.VMEM((2, pair, columns), F32),
                pltpu.VMEM((pair, columns), F32),
                dma((6,)),
                dma((2 * (n_z - 1),)),
                dma((n_pieces * (n_z - 1),)),
                dma((n_z - 1,)),
                dma((2 * (n_z - 1),)),
                dma,
                dma,
                dma((max(n_x - 1, 1),)),
                dma((max(n_x - 1, 1),)),
                dma((3,)),
                dma((3,)),
                dma,
                dma((5,)),
                pltpu.VMEM((max(rows // 16, 8), columns), F32),
                dma((2,)),
                dma((2,)),
                dma((2,)),
                dma,
                dma,
                dma,
            ],
            compiler_params=pltpu.CompilerParams(
                collective_id=0, has_side_effects=True, vmem_limit_bytes=32 * 2**20
            ),
            cost_estimate=pl.CostEstimate(
                flops=flops, bytes_accessed=8 * slab.size, transcendentals=0
            ),
        )(
            *(
                pltpu.with_memory_space_constraint(a, pltpu.HBM)
                for a in (slab, panel, pivots, pivots.reshape(1, nb), inv_lower, inv_upper)
            )
        )

    return jax.shard_map(
        local,
        mesh=mesh,
        in_specs=(P("prow", "pcol"), P(("prow", "pcol"), None), P(), P(), P()),
        out_specs=P("prow", "pcol"),
        check_vma=False,
    )
```

```python
import functools

import jax
import jax.numpy as jnp
from jax import lax
from jax.experimental import pallas as pl
from jax.experimental.pallas import tpu as pltpu
from jax.sharding import PartitionSpec as P

MESH = pl.DeviceIdType.MESH
HIGHEST = lax.Precision.HIGHEST
F32 = jnp.float32
BF16 = jnp.bfloat16


def dot(a, b):
    return jnp.dot(a, b, precision=HIGHEST, preferred_element_type=F32)


def split(a):
    high = a.astype(BF16)
    return high, (a - high.astype(F32)).astype(BF16)


def dot_split(a_high, a_low, b_high, b_low):
    rows = a_high.shape[0]
    both = jnp.dot(
        jnp.concatenate([a_high, a_low], axis=0), b_high, preferred_element_type=F32
    )
    cross = jnp.dot(a_high, b_low, preferred_element_type=F32)
    return both[:rows] + (both[rows:] + cross)


def kernel(
    n_x, n_z, early,
    slab_ref, panel_ref, pivots_ref, pivot_row_ref, inv_lower_ref, inv_upper_ref,
    out_ref,
    raw, raw_peer, lower, stage, landed, inv_lower, inv_upper, inv_split,
    picked, partner_part, chip_sum, from_x, total, halves, upper, pivots, pivot_row,
    guest, guest_split, direct, direct_landed,
    load_sem, link_send, link_recv, product_send, product_recv,
    pick_send, pick_recv, x_send, x_recv, half_send, half_recv, peer_send, peer_recv,
    detour, bridge, bridge_send, bridge_recv, onward_recv, guest_send, guest_recv, direct_send, direct_recv, detour_send, detour_recv,
):
    slab = out_ref
    prow = lax.axis_index("prow")
    pcol = lax.axis_index("pcol")
    x, core = prow // 2, prow % 2
    z, y = pcol // 2, pcol % 2
    rows, nb = panel_ref.shape
    unit = rows // 8
    step_rows = rows // 16
    pieces, edge = [], 0
    for size in (4, 4, 3, 3, 2):
        pieces.append((edge, size * step_rows))
        edge += size * step_rows
    groups = [(0, pieces[3][0]), (pieces[3][0], rows - pieces[3][0])]
    late = (3, 4)
    late_start = pieces[late[0]][0]
    late_span = pl.ds(late_start, rows - late_start)
    peer_pieces = [(0, 2 * unit), (2 * unit, 2 * unit), (4 * unit, unit)]
    peer_pieces += [(5 * unit, unit), (6 * unit, 2 * unit)]
    chunk = 2 * unit
    row_count, columns = slab_ref.shape
    half = columns // 2
    first_row = prow * row_count
    partner = {"prow": x * 2 + 1 - core}
    peer = {"pcol": z * 2 + 1 - y}
    left = {"pcol": (z - 1) * 2 + y}
    right = {"pcol": (z + 1) * 2 + y}
    has_left, has_right = z > 0, z < n_z - 1
    others = [{"prow": lax.rem(x + o, n_x) * 2 + core} for o in range(1, n_x)]

    barrier = pltpu.get_barrier_semaphore()
    for exists, device in ((has_left, left), (has_right, right)):
        @pl.when(exists)
        def _():
            pl.semaphore_signal(barrier, inc=1, device_id=device, device_id_type=MESH)
    fixed = [peer] + others + [partner]
    for device in fixed:
        pl.semaphore_signal(barrier, inc=1, device_id=device, device_id_type=MESH)

    panel_load = pltpu.make_async_copy(panel_ref, raw.at[z], load_sem.at[0])
    slab_load = pltpu.make_async_copy(slab_ref, slab, load_sem.at[1])
    upper_load = pltpu.make_async_copy(inv_upper_ref, inv_upper, load_sem.at[2])
    lower_load = pltpu.make_async_copy(inv_lower_ref, inv_lower, load_sem.at[3])
    pivot_load = pltpu.make_async_copy(pivots_ref, pivots, load_sem.at[4])
    pivot_row_load = pltpu.make_async_copy(pivot_row_ref, pivot_row, load_sem.at[5])
    for load in (panel_load, pivot_load, slab_load, pivot_row_load, upper_load, lower_load):
        load.start()

    def remote(source, target, send_sem, recv_sem, device):
        return pltpu.make_async_remote_copy(
            src_ref=source, dst_ref=target, send_sem=send_sem, recv_sem=recv_sem,
            device_id=device, device_id_type=MESH,
        )

    def span_of(start, count):
        return pl.ds(pl.multiple_of(start, 8), count)

    def block_at(direction, distance):
        return z - distance if direction == 0 else z + distance

    def receives(direction, distance):
        block = block_at(direction, distance)
        return block >= 0 if direction == 0 else block < n_z

    def sends(direction, distance):
        exists = has_right if direction == 0 else has_left
        return exists & receives(direction, distance)

    def guest_of(direction):
        return z == n_z - 1 if direction == 0 else z == 0

    def host_of(direction):
        return z == n_z - 2 if direction == 0 else z == 1

    def comes(direction, distance, g):
        exists = receives(direction, distance)
        if g in late:
            exists &= ~(guest_of(direction) & (distance == 1))
        return exists

    def goes(direction, g):
        exists = sends(direction, 0)
        if g in late:
            exists &= ~host_of(direction)
        return exists

    def link(direction, distance, g):
        block = block_at(direction, distance)
        spot = raw.at[block, pl.ds(*pieces[g])]
        return remote(
            spot, spot, link_send.at[direction * (n_z - 1) + distance % (n_z - 1)],
            link_recv.at[(block - direction) * len(pieces) + g],
            right if direction == 0 else left,
        )

    def peer_copy(i):
        span = pl.ds(*peer_pieces[i])
        return remote(
            raw.at[z, span], raw_peer.at[span], peer_send, peer_recv.at[i], peer
        )

    panel_load.wait()
    n_peers = len(fixed) + has_left.astype(jnp.int32) + has_right.astype(jnp.int32)
    pl.semaphore_wait(barrier, n_peers)
    for g in range(len(pieces)):
        for direction in (0, 1):
            @pl.when(goes(direction, g))
            def _():
                link(direction, 0, g).start()

    for i in range(3):
        peer_copy(i).start()

    pivot_load.wait()
    slab_load.wait()

    def pick(k, carry):
        local = pivots[k] - first_row
        inside = (local >= 0) & (local < row_count)
        row = slab[pl.ds(jnp.where(inside, local, 0), 1), :]
        row = jnp.where(inside, row, 0.0)
        picked[0, pl.ds(k, 1), :] = row[:, :half]
        picked[1, pl.ds(k, 1), :] = row[:, half:]
        return carry

    lax.fori_loop(0, nb, pick, 0, unroll=8)

    pick_copy = remote(picked.at[1 - core], partner_part, pick_send, pick_recv, partner)
    pick_copy.start()
    pivot_row_load.wait()
    upper_load.wait()
    lower_load.wait()
    inv_split[0], inv_split[1] = split(inv_upper[...])
    pick_copy.wait()
    chip_sum[...] = picked[core] + partner_part[...]
    x_copies = [
        remote(chip_sum, from_x.at[i], x_send.at[i], x_recv.at[i], device)
        for i, device in enumerate(others)
    ]
    for copy in x_copies:
        copy.start()

    def pivot_hits(start, count):
        ids = first_row + start + lax.broadcasted_iota(jnp.int32, (count, nb), 0)
        return jnp.where(ids == pivot_row[...], 1.0, 0.0)

    def is_pivot(hits):
        return jnp.max(hits, axis=1, keepdims=True) > 0.0

    def solve(rows_in, hits):
        high, low = split(rows_in)
        solved = dot_split(high, low, inv_split[0], inv_split[1])
        return split(jnp.where(is_pivot(hits), -hits, solved))

    def clear(i, carry):
        start = i * 2 * chunk
        span = span_of(start, 2 * chunk)
        slab[span, :] = jnp.where(
            is_pivot(pivot_hits(start, 2 * chunk)), 0.0, slab[span, :]
        )
        return carry

    lax.fori_loop(0, row_count // (2 * chunk), clear, 0)

    def solve_rows(block, start, count):
        span = span_of(start, count)
        hits = pivot_hits((block * 2 + y) * rows + start, count)
        high, low = solve(raw[block, span, :], hits)
        lower[0, block, span, :] = high
        lower[1, block, span, :] = low

    def prepare(distance, g):
        for direction in (0, 1):
            arrives = comes(direction, distance, g)

            @pl.when(arrives)
            def _():
                link(direction, distance, g).wait_recv()

            @pl.when(arrives & sends(direction, distance))
            def _():
                link(direction, distance, g).start()

            @pl.when(arrives)
            def _():
                solve_rows(block_at(direction, distance), *pieces[g])

    for g in range(early[0]):
        prepare(1, g)

    for copy in x_copies:
        copy.wait()
    summed = chip_sum[...]
    for o in range(1, n_x):
        summed = summed + from_x[o - 1]
    total[...] = summed
    halves[core] = dot(inv_lower[...], total[...])
    to_peer = remote(
        halves.at[core], halves.at[2 + core], half_send.at[0], half_recv.at[0], peer
    )
    to_partner = remote(
        halves.at[core], halves.at[core], half_send.at[1], half_recv.at[1], partner
    )
    to_peer.start()
    to_partner.start()
    peer_copy(3).start()

    def solve_own(g, carry):
        solve_rows(z, g * chunk, chunk)
        return carry

    lax.fori_loop(0, rows // chunk, solve_own, 0)
    for g in range(early[0], early[1]):
        prepare(1, g)

    to_peer.wait()
    onward = remote(
        halves.at[2 + core], halves.at[2 + core], half_send.at[2], half_recv.at[2], partner
    )
    onward.start()
    to_partner.wait()

    def split_upper(i):
        span = slice(i * half, (i + 1) * half)
        upper[0, :, span], upper[1, :, span] = split(halves[i])

    split_upper(0)
    split_upper(1)
    onward.wait()
    split_upper(2)
    split_upper(3)

    def guest_copy(direction):
        return remote(
            halves.at[0:2], guest.at[direction], guest_send.at[direction],
            guest_recv.at[direction], left if direction == 0 else right,
        )

    full = direct_landed.shape[0]
    kept = full - detour.shape[0]
    first = (x == 0) & (y == 0) & (n_x > 1)
    helper = (x == 1) & (y == 0)

    moved = bridge.shape[1]

    def direct_copy(direction, count, start):
        span = pl.ds(start, count - start)
        return remote(
            direct.at[direction, span], direct_landed.at[span],
            direct_send.at[direction], direct_recv,
            right if direction == 0 else left,
        )

    def bridge_copy(direction):
        return remote(
            direct.at[direction, pl.ds(0, moved)], bridge.at[direction],
            bridge_send.at[direction], bridge_recv.at[direction], partner,
        )

    def bridge_onward(direction):
        column = right if direction == 0 else left
        return remote(
            bridge.at[direction], direct_landed.at[pl.ds(0, moved)],
            bridge_send.at[direction], onward_recv, {**partner, **column},
        )

    def by_core(action, direction, count):
        pl.when(core == 0)(lambda: getattr(direct_copy(direction, count, moved), action)())
        pl.when(core != 0)(lambda: getattr(direct_copy(direction, count, 0), action)())

    def detour_copy(leg):
        source = direct.at[1, pl.ds(kept, full - kept)] if leg == 0 else detour
        target = direct_landed.at[pl.ds(kept, full - kept)] if leg == 2 else detour
        device = ({"prow": 2 + core}, left, {"prow": core})[leg]
        return remote(source, target, detour_send, detour_recv, device)

    def of_first(direction):
        return first if direction == 1 else x < 0

    for direction in (0, 1):
        @pl.when(guest_of(direction))
        def _():
            guest_copy(direction).start()

    def product_copy(direction, distance, g):
        block = block_at(direction, distance)
        span = pl.ds(*pieces[g])
        return remote(
            stage.at[block, span], landed.at[block, span],
            product_send.at[block - direction],
            product_recv.at[(block - direction) * 2 + g // 3], peer,
        )

    def subtract(block, side, start, count, product):
        span = span_of((block * 2 + side) * rows + start, count)
        slab[span, :] = slab[span, :] - product

    def multiply(distance, g):
        start, count = pieces[g]
        span = pl.ds(start, count)
        for direction in (0, 1):
            @pl.when(comes(direction, distance, g))
            def _():
                block = block_at(direction, distance)
                products = dot_split(
                    lower[0, block, span, :], lower[1, block, span, :],
                    upper[0], upper[1],
                )
                stage[block, span, :] = products[:, columns:]
                product_copy(direction, distance, g).start()
                subtract(block, y, start, count, products[:, :columns])

    def take(distance, group):
        start, count = groups[group]
        for direction in (0, 1):
            @pl.when(comes(direction, distance, 3 * group))
            def _():
                block = block_at(direction, distance)
                landing = landed.at[block, pl.ds(start, count)]
                remote(
                    landing, landing, product_send.at[block - direction],
                    product_recv.at[(block - direction) * 2 + group], peer,
                ).wait_recv()
                subtract(
                    block, 1 - y, start, count, landed[block, pl.ds(start, count), :]
                )

    def multiply_own(i, carry):
        span = span_of(i * chunk, chunk)
        product = dot_split(
            lower[0, z, span, :], lower[1, z, span, :],
            upper[0, :, :columns], upper[1, :, :columns],
        )
        subtract(z, y, i * chunk, chunk, product)
        return carry

    def solve_peer(start, count):
        hits = pivot_hits((z * 2 + 1 - y) * rows + start, count)
        return solve(raw_peer[pl.ds(start, count), :], hits)

    def multiply_peer(i):
        for c in ((0,), (1,), (2, 3), (4,))[i]:
            peer_copy(c).wait_recv()
        high, low = solve_peer(i * chunk, chunk)
        product = dot_split(high, low, upper[0, :, :columns], upper[1, :, :columns])
        subtract(z, 1 - y, i * chunk, chunk, product)

    def serve():
        for direction in (0, 1):
            @pl.when(host_of(direction))
            def _():
                guest_copy(direction).wait_recv()
                for i in (0, 1):
                    span = slice(i * half, (i + 1) * half)
                    guest_split[0, :, span], guest_split[1, :, span] = split(
                        guest[direction, i]
                    )
                high, low = solve_peer(late_start, rows - late_start)
                direct[direction] = dot_split(
                    jnp.concatenate([lower[0, z, late_span, :], high], axis=0),
                    jnp.concatenate([lower[1, z, late_span, :], low], axis=0),
                    guest_split[0], guest_split[1],
                )
                if direction == 1:
                    @pl.when(first)
                    def _():
                        detour_copy(0).start()

                    @pl.when(helper)
                    def _():
                        detour_copy(0).wait_recv()
                        detour_copy(1).start()

    def start_direct():
        for direction in (0, 1):
            @pl.when(host_of(direction) & (core == 0))
            def _():
                bridge_copy(direction).start()

            @pl.when(host_of(direction) & (core != 0))
            def _():
                bridge_copy(direction).wait_recv()
                bridge_onward(direction).start()

            @pl.when(host_of(direction) & of_first(direction))
            def _():
                by_core("start", direction, kept)

            @pl.when(host_of(direction) & ~of_first(direction))
            def _():
                by_core("start", direction, full)

    for g in range(early[1]):
        multiply(1, g)
    peer_copy(4).start()
    for g in range(early[1], len(pieces)):
        prepare(1, g)
        multiply(1, g)
        lax.fori_loop(2 * (g - early[1]), 2 * (g - early[1]) + 2, multiply_own, 0)

    def pass_detour():
        @pl.when(guest_of(1) & helper)
        def _():
            detour_copy(1).wait_recv()
            detour_copy(2).start()

    def step(distance, final_step):
        for g in range(len(pieces)):
            prepare(distance, g)
            multiply(distance, g)
            if isinstance(distance, int) and not final_step and g < 4:
                multiply_peer(g)
            if isinstance(distance, int) and not final_step and g == 3:
                serve()
            if g in (2, 4):
                take(distance - 1, g // 4)
            if final_step and g == 3:
                pass_detour()
            if final_step and g == 4:
                take(distance, 0)

    if n_z <= 3:
        for i in range(4):
            multiply_peer(i)
    if n_z > 3:
        step(2, False)
        lax.fori_loop(3, n_z - 1, lambda d, c: (step(d, False), c)[1], 0)
    if n_z <= 3:
        serve()
    start_direct()
    if n_z > 2:
        step(n_z - 1, True)
    else:
        pass_detour()

    def settle_products(direction, distance):
        block = block_at(direction, distance)

        def wait(count):
            span = pl.ds(0, count)
            remote(
                stage.at[block, span], landed.at[block, span],
                product_send.at[block - direction], product_recv.at[0], peer,
            ).wait_send()

        whole = receives(direction, distance)
        short = guest_of(direction) & (distance == 1)
        pl.when(whole & ~short)(lambda: wait(rows))
        pl.when(whole & short)(lambda: wait(late_start))

    def settle_links(direction, distance):
        block = block_at(direction, distance)

        def wait(count):
            spot = raw.at[block, pl.ds(0, count)]
            remote(
                spot, spot, link_send.at[direction * (n_z - 1) + distance % (n_z - 1)], link_recv.at[0],
                right if direction == 0 else left,
            ).wait_send()

        whole = sends(direction, distance)
        short = host_of(direction) & (distance == 0)
        pl.when(whole & ~short)(lambda: wait(rows))
        pl.when(whole & short)(lambda: wait(late_start))

    def settle(distance, carry):
        for direction in (0, 1):
            settle_links(direction, distance)
        return carry

    lax.fori_loop(0, n_z - 1, settle, 0)
    remote(raw.at[z], raw_peer, peer_send, peer_recv.at[0], peer).wait_send()
    for direction in (0, 1):
        @pl.when(guest_of(direction))
        def _():
            guest_copy(direction).wait_send()
    for group in range(1 if n_z > 2 else 0, 2):
        take(n_z - 1, group)

    def settle_late(distance, carry):
        for direction in (0, 1):
            settle_products(direction, distance)
        return carry

    for direction in (0, 1):
        pl.when(host_of(direction) & (core == 0))(lambda: bridge_copy(direction).wait_send())
        pl.when(host_of(direction) & (core != 0))(lambda: bridge_onward(direction).wait_send())

    lax.fori_loop(1, n_z, settle_late, 0)
    for direction in (0, 1):
        @pl.when(host_of(direction))
        def _():
            @pl.when(of_first(direction))
            def _():
                by_core("wait_send", direction, kept)
                detour_copy(0).wait_send()

            @pl.when(~of_first(direction))
            def _():
                by_core("wait_send", direction, full)

            if direction == 1:
                @pl.when(helper)
                def _():
                    detour_copy(1).wait_send()

        @pl.when(guest_of(direction))
        def _():
            @pl.when(of_first(direction))
            def _():
                by_core("wait_recv", direction, kept)
                detour_copy(2).wait_recv()

            @pl.when(~of_first(direction))
            def _():
                by_core("wait_recv", direction, full)

            if direction == 1:
                @pl.when(helper)
                def _():
                    detour_copy(2).wait_send()

            pl.when(core == 0)(lambda: bridge_onward(direction).wait_recv())
            count = rows - late_start
            block = block_at(direction, 1)
            subtract(block, y, late_start, count, direct_landed[:count])
            subtract(block, 1 - y, late_start, count, direct_landed[count:])


def solution(mesh):
    n_prow, n_pcol = mesh.shape["prow"], mesh.shape["pcol"]
    n_x, n_z, n_pieces, early = n_prow // 2, n_pcol // 2, 5, (1, 3)

    def local(slab, panel, pivots, inv_lower, inv_upper):
        (row_count, columns), (rows, nb) = slab.shape, panel.shape
        half = columns // 2
        pair = rows * 5 // 8
        hbm = pl.BlockSpec(memory_space=pltpu.HBM)
        dma = pltpu.SemaphoreType.DMA
        flops = 2 * row_count * nb * (nb + columns)
        return pl.pallas_call(
            functools.partial(kernel, n_x, n_z, early),
            out_shape=pltpu.VMEM(slab.shape, slab.dtype),
            in_specs=[
                hbm,
                hbm,
                hbm,
                hbm,
                hbm,
                hbm,
            ],
            out_specs=pl.BlockSpec(memory_space=pltpu.VMEM),
            scratch_shapes=[
                pltpu.VMEM((n_z, rows, nb), F32),
                pltpu.VMEM((rows, nb), F32),
                pltpu.VMEM((2, n_z, rows, nb), BF16),
                pltpu.VMEM((n_z, rows, columns), F32),
                pltpu.VMEM((n_z, rows, columns), F32),
                pltpu.VMEM((nb, nb), F32),
                pltpu.VMEM((nb, nb), F32),
                pltpu.VMEM((2, nb, nb), BF16),
                pltpu.VMEM((2, nb, half), F32),
                pltpu.VMEM((nb, half), F32),
                pltpu.VMEM((nb, half), F32),
                pltpu.VMEM((max(n_x - 1, 1), nb, half), F32),
                pltpu.VMEM((nb, half), F32),
                pltpu.VMEM((4, nb, half), F32),
                pltpu.VMEM((2, nb, 2 * columns), BF16),
                pltpu.SMEM((nb,), jnp.int32),
                pltpu.VMEM((1, nb), jnp.int32),
                pltpu.VMEM((2, 2, nb, half), F32),
                pltpu.VMEM((2, nb, columns), BF16),
                pltpu.VMEM((2, pair, columns), F32),
                pltpu.VMEM((pair, columns), F32),
                dma((6,)),
                dma((2 * (n_z - 1),)),
                dma((n_pieces * (n_z - 1),)),
                dma((n_z - 1,)),
                dma((2 * (n_z - 1),)),
                dma,
                dma,
                dma((max(n_x - 1, 1),)),
                dma((max(n_x - 1, 1),)),
                dma((3,)),
                dma((3,)),
                dma,
                dma((5,)),
                pltpu.VMEM((max(rows // 16, 8), columns), F32),
                pltpu.VMEM((2, rows // 8, columns), F32),
                dma((2,)),
                dma((2,)),
                dma,
                dma((2,)),
                dma((2,)),
                dma((2,)),
                dma,
                dma,
                dma,
            ],
            compiler_params=pltpu.CompilerParams(
                collective_id=0, has_side_effects=True, vmem_limit_bytes=32 * 2**20
            ),
            cost_estimate=pl.CostEstimate(
                flops=flops, bytes_accessed=8 * slab.size, transcendentals=0
            ),
        )(
            *(
                pltpu.with_memory_space_constraint(a, pltpu.HBM)
                for a in (slab, panel, pivots, pivots.reshape(1, nb), inv_lower, inv_upper)
            )
        )

    return jax.shard_map(
        local,
        mesh=mesh,
        in_specs=(P("prow", "pcol"), P(("prow", "pcol"), None), P(), P(), P()),
        out_specs=P("prow", "pcol"),
        check_vma=False,
    )
```

```python
import functools

import jax
import jax.numpy as jnp
from jax import lax
from jax.experimental import pallas as pl
from jax.experimental.pallas import tpu as pltpu
from jax.sharding import PartitionSpec as P

MESH = pl.DeviceIdType.MESH
HIGHEST = lax.Precision.HIGHEST
F32 = jnp.float32
BF16 = jnp.bfloat16


def dot(a, b):
    return jnp.dot(a, b, precision=HIGHEST, preferred_element_type=F32)


def split(a):
    high = a.astype(BF16)
    return high, (a - high.astype(F32)).astype(BF16)


def dot_split(a_high, a_low, b_high, b_low):
    rows = a_high.shape[0]
    both = jnp.dot(
        jnp.concatenate([a_high, a_low], axis=0), b_high, preferred_element_type=F32
    )
    cross = jnp.dot(a_high, b_low, preferred_element_type=F32)
    return both[:rows] + (both[rows:] + cross)


def kernel(
    n_x, n_z, early,
    slab_ref, panel_ref, pivots_ref, pivot_row_ref, inv_lower_ref, inv_upper_ref,
    out_ref,
    raw, raw_peer, lower, stage, landed, inv_lower, inv_upper, inv_split,
    picked, partner_part, chip_sum, from_x, total, halves, upper, pivots, pivot_row,
    guest, guest_split, direct, direct_landed,
    load_sem, link_send, link_recv, product_send, product_recv,
    pick_send, pick_recv, x_send, x_recv, half_send, half_recv, peer_send, peer_recv,
    detour, bridge, bridge_send, bridge_recv, onward_recv, guest_send, guest_recv, direct_send, direct_recv, detour_send, detour_recv,
):
    slab = out_ref
    prow = lax.axis_index("prow")
    pcol = lax.axis_index("pcol")
    x, core = prow // 2, prow % 2
    z, y = pcol // 2, pcol % 2
    rows, nb = panel_ref.shape
    unit = rows // 8
    step_rows = rows // 16
    pieces, edge = [], 0
    for size in (4, 4, 3, 3, 2):
        pieces.append((edge, size * step_rows))
        edge += size * step_rows
    groups = [(0, pieces[3][0]), (pieces[3][0], rows - pieces[3][0])]
    late = (3, 4)
    late_start = pieces[late[0]][0]
    late_span = pl.ds(late_start, rows - late_start)
    peer_pieces = [(0, 2 * unit), (2 * unit, 2 * unit), (4 * unit, unit)]
    peer_pieces += [(5 * unit, unit), (6 * unit, 2 * unit)]
    chunk = 2 * unit
    row_count, columns = slab_ref.shape
    half = columns // 2
    first_row = prow * row_count
    partner = {"prow": x * 2 + 1 - core}
    peer = {"pcol": z * 2 + 1 - y}
    left = {"pcol": (z - 1) * 2 + y}
    right = {"pcol": (z + 1) * 2 + y}
    has_left, has_right = z > 0, z < n_z - 1
    others = [{"prow": lax.rem(x + o, n_x) * 2 + core} for o in range(1, n_x)]

    barrier = pltpu.get_barrier_semaphore()
    for exists, device in ((has_left, left), (has_right, right)):
        @pl.when(exists)
        def _():
            pl.semaphore_signal(barrier, inc=1, device_id=device, device_id_type=MESH)
    fixed = [peer] + others + [partner]
    for device in fixed:
        pl.semaphore_signal(barrier, inc=1, device_id=device, device_id_type=MESH)

    panel_load = pltpu.make_async_copy(panel_ref, raw.at[z], load_sem.at[0])
    slab_load = pltpu.make_async_copy(slab_ref, slab, load_sem.at[1])
    upper_load = pltpu.make_async_copy(inv_upper_ref, inv_upper, load_sem.at[2])
    lower_load = pltpu.make_async_copy(inv_lower_ref, inv_lower, load_sem.at[3])
    pivot_load = pltpu.make_async_copy(pivots_ref, pivots, load_sem.at[4])
    pivot_row_load = pltpu.make_async_copy(pivot_row_ref, pivot_row, load_sem.at[5])
    for load in (panel_load, pivot_load, slab_load, pivot_row_load, upper_load, lower_load):
        load.start()

    def remote(source, target, send_sem, recv_sem, device):
        return pltpu.make_async_remote_copy(
            src_ref=source, dst_ref=target, send_sem=send_sem, recv_sem=recv_sem,
            device_id=device, device_id_type=MESH,
        )

    def span_of(start, count):
        return pl.ds(pl.multiple_of(start, 8), count)

    def block_at(direction, distance):
        return z - distance if direction == 0 else z + distance

    def receives(direction, distance):
        block = block_at(direction, distance)
        return block >= 0 if direction == 0 else block < n_z

    def sends(direction, distance):
        exists = has_right if direction == 0 else has_left
        return exists & receives(direction, distance)

    def guest_of(direction):
        return z == n_z - 1 if direction == 0 else z == 0

    def host_of(direction):
        return z == n_z - 2 if direction == 0 else z == 1

    def comes(direction, distance, g):
        exists = receives(direction, distance)
        if g in late:
            exists &= ~(guest_of(direction) & (distance == 1))
        return exists

    def goes(direction, g):
        exists = sends(direction, 0)
        if g in late:
            exists &= ~host_of(direction)
        return exists

    def link(direction, distance, g):
        block = block_at(direction, distance)
        spot = raw.at[block, pl.ds(*pieces[g])]
        return remote(
            spot, spot, link_send.at[direction * (n_z - 1) + distance % (n_z - 1)],
            link_recv.at[(block - direction) * len(pieces) + g],
            right if direction == 0 else left,
        )

    def peer_copy(i):
        span = pl.ds(*peer_pieces[i])
        return remote(
            raw.at[z, span], raw_peer.at[span], peer_send, peer_recv.at[i], peer
        )

    panel_load.wait()
    slots = guest_send.shape[0]
    n_peers = len(fixed) + has_left.astype(jnp.int32) + has_right.astype(jnp.int32)
    pl.semaphore_wait(barrier, n_peers)
    for g in range(len(pieces)):
        for direction in (0, 1):
            @pl.when(goes(direction, g))
            def _():
                link(direction, 0, g).start()

    for i in range(3):
        peer_copy(i).start()

    pivot_load.wait()
    slab_load.wait()

    def pick(k, carry):
        local = pivots[k] - first_row
        inside = (local >= 0) & (local < row_count)
        row = slab[pl.ds(jnp.where(inside, local, 0), 1), :]
        row = jnp.where(inside, row, 0.0)
        picked[0, pl.ds(k, 1), :] = row[:, :half]
        picked[1, pl.ds(k, 1), :] = row[:, half:]
        return carry

    lax.fori_loop(0, nb, pick, 0, unroll=8)

    pick_copy = remote(picked.at[1 - core], partner_part, pick_send, pick_recv, partner)
    pick_copy.start()
    pivot_row_load.wait()
    upper_load.wait()
    lower_load.wait()
    inv_split[0], inv_split[1] = split(inv_upper[...])
    pick_copy.wait()
    chip_sum[...] = picked[core] + partner_part[...]
    x_copies = [
        remote(chip_sum, from_x.at[i], x_send.at[i], x_recv.at[i], device)
        for i, device in enumerate(others)
    ]
    for copy in x_copies:
        copy.start()

    def pivot_hits(start, count):
        ids = first_row + start + lax.broadcasted_iota(jnp.int32, (count, nb), 0)
        return jnp.where(ids == pivot_row[...], 1.0, 0.0)

    def is_pivot(hits):
        return jnp.max(hits, axis=1, keepdims=True) > 0.0

    def solve(rows_in, hits):
        high, low = split(rows_in)
        solved = dot_split(high, low, inv_split[0], inv_split[1])
        return split(jnp.where(is_pivot(hits), -hits, solved))

    def clear(i, carry):
        start = i * 2 * chunk
        span = span_of(start, 2 * chunk)
        slab[span, :] = jnp.where(
            is_pivot(pivot_hits(start, 2 * chunk)), 0.0, slab[span, :]
        )
        return carry

    lax.fori_loop(0, row_count // (2 * chunk), clear, 0)

    def solve_rows(block, start, count):
        span = span_of(start, count)
        hits = pivot_hits((block * 2 + y) * rows + start, count)
        high, low = solve(raw[block, span, :], hits)
        lower[0, block, span, :] = high
        lower[1, block, span, :] = low

    def prepare(distance, g):
        for direction in (0, 1):
            arrives = comes(direction, distance, g)

            @pl.when(arrives)
            def _():
                link(direction, distance, g).wait_recv()

            @pl.when(arrives & sends(direction, distance))
            def _():
                link(direction, distance, g).start()

            @pl.when(arrives)
            def _():
                solve_rows(block_at(direction, distance), *pieces[g])

    for g in range(early[0]):
        prepare(1, g)

    for copy in x_copies:
        copy.wait()
    summed = chip_sum[...]
    for o in range(1, n_x):
        summed = summed + from_x[o - 1]
    total[...] = summed
    halves[core] = dot(inv_lower[...], total[...])
    to_peer = remote(
        halves.at[core], halves.at[2 + core], half_send.at[0], half_recv.at[0], peer
    )
    to_partner = remote(
        halves.at[core], halves.at[core], half_send.at[1], half_recv.at[1], partner
    )
    to_peer.start()
    to_partner.start()
    peer_copy(3).start()

    def solve_own(g, carry):
        solve_rows(z, g * chunk, chunk)
        return carry

    lax.fori_loop(0, rows // chunk, solve_own, 0)
    for g in range(early[0], early[1]):
        prepare(1, g)

    to_peer.wait()
    onward = remote(
        halves.at[2 + core], halves.at[2 + core], half_send.at[2], half_recv.at[2], partner
    )
    onward.start()
    to_partner.wait()

    def split_upper(i):
        span = slice(i * half, (i + 1) * half)
        upper[0, :, span], upper[1, :, span] = split(halves[i])

    split_upper(0)
    split_upper(1)
    onward.wait()
    split_upper(2)
    split_upper(3)

    def guest_copy(direction):
        return remote(
            halves.at[0:2], guest.at[direction], guest_send.at[direction % slots],
            guest_recv.at[direction % slots], left if direction == 0 else right,
        )

    full = direct_landed.shape[0]
    kept = full - detour.shape[0]
    first = (x == 0) & (y == 0) & (n_x > 1)
    helper = (x == 1) & (y == 0)

    moved = bridge.shape[1]

    def direct_copy(direction, count, start):
        span = pl.ds(start, count - start)
        return remote(
            direct.at[direction, span], direct_landed.at[span],
            direct_send.at[direction % slots], direct_recv,
            right if direction == 0 else left,
        )

    def bridge_copy(direction):
        return remote(
            direct.at[direction, pl.ds(0, moved)], bridge.at[direction],
            bridge_send.at[direction % slots], bridge_recv.at[direction % slots], partner,
        )

    def bridge_onward(direction):
        column = right if direction == 0 else left
        return remote(
            bridge.at[direction], direct_landed.at[pl.ds(0, moved)],
            bridge_send.at[direction % slots], onward_recv, {**partner, **column},
        )

    def by_core(action, direction, count):
        pl.when(core == 0)(lambda: getattr(direct_copy(direction, count, moved), action)())
        pl.when(core != 0)(lambda: getattr(direct_copy(direction, count, 0), action)())

    def detour_copy(leg):
        source = direct.at[1, pl.ds(kept, full - kept)] if leg == 0 else detour
        target = direct_landed.at[pl.ds(kept, full - kept)] if leg == 2 else detour
        device = ({"prow": 2 + core}, left, {"prow": core})[leg]
        return remote(source, target, detour_send, detour_recv, device)

    def of_first(direction):
        return first if direction == 1 else x < 0

    for direction in (0, 1):
        @pl.when(guest_of(direction))
        def _():
            guest_copy(direction).start()

    def product_copy(direction, distance, g):
        block = block_at(direction, distance)
        span = pl.ds(*pieces[g])
        return remote(
            stage.at[block, span], landed.at[block, span],
            product_send.at[block - direction],
            product_recv.at[(block - direction) * 2 + g // 3], peer,
        )

    def subtract(block, side, start, count, product):
        span = span_of((block * 2 + side) * rows + start, count)
        slab[span, :] = slab[span, :] - product

    def multiply(distance, g):
        start, count = pieces[g]
        span = pl.ds(start, count)
        for direction in (0, 1):
            @pl.when(comes(direction, distance, g))
            def _():
                block = block_at(direction, distance)
                products = dot_split(
                    lower[0, block, span, :], lower[1, block, span, :],
                    upper[0], upper[1],
                )
                stage[block, span, :] = products[:, columns:]
                product_copy(direction, distance, g).start()
                subtract(block, y, start, count, products[:, :columns])

    def take(distance, group):
        start, count = groups[group]
        for direction in (0, 1):
            @pl.when(comes(direction, distance, 3 * group))
            def _():
                block = block_at(direction, distance)
                landing = landed.at[block, pl.ds(start, count)]
                remote(
                    landing, landing, product_send.at[block - direction],
                    product_recv.at[(block - direction) * 2 + group], peer,
                ).wait_recv()
                subtract(
                    block, 1 - y, start, count, landed[block, pl.ds(start, count), :]
                )

    def multiply_own(i, carry):
        span = span_of(i * chunk, chunk)
        product = dot_split(
            lower[0, z, span, :], lower[1, z, span, :],
            upper[0, :, :columns], upper[1, :, :columns],
        )
        subtract(z, y, i * chunk, chunk, product)
        return carry

    def solve_peer(start, count):
        hits = pivot_hits((z * 2 + 1 - y) * rows + start, count)
        return solve(raw_peer[pl.ds(start, count), :], hits)

    def multiply_peer(i):
        for c in ((0,), (1,), (2, 3), (4,))[i]:
            peer_copy(c).wait_recv()
        high, low = solve_peer(i * chunk, chunk)
        product = dot_split(high, low, upper[0, :, :columns], upper[1, :, :columns])
        subtract(z, 1 - y, i * chunk, chunk, product)

    def serve():
        for direction in (0, 1):
            @pl.when(host_of(direction))
            def _():
                guest_copy(direction).wait_recv()
                for i in (0, 1):
                    span = slice(i * half, (i + 1) * half)
                    guest_split[0, :, span], guest_split[1, :, span] = split(
                        guest[direction, i]
                    )
                high, low = solve_peer(late_start, rows - late_start)
                direct[direction] = dot_split(
                    jnp.concatenate([lower[0, z, late_span, :], high], axis=0),
                    jnp.concatenate([lower[1, z, late_span, :], low], axis=0),
                    guest_split[0], guest_split[1],
                )
                if direction == 1:
                    @pl.when(first)
                    def _():
                        detour_copy(0).start()

                    @pl.when(helper)
                    def _():
                        detour_copy(0).wait_recv()
                        detour_copy(1).start()

    def start_direct():
        for direction in (0, 1):
            @pl.when(host_of(direction) & (core == 0))
            def _():
                bridge_copy(direction).start()

            @pl.when(host_of(direction) & (core != 0))
            def _():
                bridge_copy(direction).wait_recv()
                bridge_onward(direction).start()

            @pl.when(host_of(direction) & of_first(direction))
            def _():
                by_core("start", direction, kept)

            @pl.when(host_of(direction) & ~of_first(direction))
            def _():
                by_core("start", direction, full)

    for g in range(early[1]):
        multiply(1, g)
    peer_copy(4).start()
    for g in range(early[1], len(pieces)):
        prepare(1, g)
        multiply(1, g)
        lax.fori_loop(2 * (g - early[1]), 2 * (g - early[1]) + 2, multiply_own, 0)

    def pass_detour():
        @pl.when(guest_of(1) & helper)
        def _():
            detour_copy(1).wait_recv()
            detour_copy(2).start()

    def step(distance, final_step):
        for g in range(len(pieces)):
            prepare(distance, g)
            multiply(distance, g)
            if isinstance(distance, int) and not final_step and g < 4:
                multiply_peer(g)
            if isinstance(distance, int) and not final_step and g == 3:
                serve()
            if g in (2, 4):
                take(distance - 1, g // 4)
            if final_step and g == 3:
                pass_detour()
            if final_step and g == 4:
                take(distance, 0)

    if n_z <= 3:
        for i in range(4):
            multiply_peer(i)
    if n_z > 3:
        step(2, False)
        lax.fori_loop(3, n_z - 1, lambda d, c: (step(d, False), c)[1], 0)
    if n_z <= 3:
        serve()
    start_direct()
    if n_z > 2:
        step(n_z - 1, True)
    else:
        pass_detour()

    def settle_products(direction, distance):
        block = block_at(direction, distance)

        def wait(count):
            span = pl.ds(0, count)
            remote(
                stage.at[block, span], landed.at[block, span],
                product_send.at[block - direction], product_recv.at[0], peer,
            ).wait_send()

        whole = receives(direction, distance)
        short = guest_of(direction) & (distance == 1)
        pl.when(whole & ~short)(lambda: wait(rows))
        pl.when(whole & short)(lambda: wait(late_start))

    def settle_links(direction, distance):
        block = block_at(direction, distance)

        def wait(count):
            spot = raw.at[block, pl.ds(0, count)]
            remote(
                spot, spot, link_send.at[direction * (n_z - 1) + distance % (n_z - 1)], link_recv.at[0],
                right if direction == 0 else left,
            ).wait_send()

        whole = sends(direction, distance)
        short = host_of(direction) & (distance == 0)
        pl.when(whole & ~short)(lambda: wait(rows))
        pl.when(whole & short)(lambda: wait(late_start))

    def settle(distance, carry):
        for direction in (0, 1):
            settle_links(direction, distance)
        return carry

    lax.fori_loop(0, n_z - 1, settle, 0)
    remote(raw.at[z], raw_peer, peer_send, peer_recv.at[0], peer).wait_send()
    for direction in (0, 1):
        @pl.when(guest_of(direction))
        def _():
            guest_copy(direction).wait_send()
    for group in range(1 if n_z > 2 else 0, 2):
        take(n_z - 1, group)

    def settle_late(distance, carry):
        for direction in (0, 1):
            settle_products(direction, distance)
        return carry

    for direction in (0, 1):
        pl.when(host_of(direction) & (core == 0))(lambda: bridge_copy(direction).wait_send())
        pl.when(host_of(direction) & (core != 0))(lambda: bridge_onward(direction).wait_send())

    lax.fori_loop(1, n_z, settle_late, 0)
    for direction in (0, 1):
        @pl.when(host_of(direction))
        def _():
            @pl.when(of_first(direction))
            def _():
                by_core("wait_send", direction, kept)
                detour_copy(0).wait_send()

            @pl.when(~of_first(direction))
            def _():
                by_core("wait_send", direction, full)

            if direction == 1:
                @pl.when(helper)
                def _():
                    detour_copy(1).wait_send()

        @pl.when(guest_of(direction))
        def _():
            @pl.when(of_first(direction))
            def _():
                by_core("wait_recv", direction, kept)
                detour_copy(2).wait_recv()

            @pl.when(~of_first(direction))
            def _():
                by_core("wait_recv", direction, full)

            if direction == 1:
                @pl.when(helper)
                def _():
                    detour_copy(2).wait_send()

            pl.when(core == 0)(lambda: bridge_onward(direction).wait_recv())
            count = rows - late_start
            block = block_at(direction, 1)
            subtract(block, y, late_start, count, direct_landed[:count])
            subtract(block, 1 - y, late_start, count, direct_landed[count:])


def solution(mesh):
    n_prow, n_pcol = mesh.shape["prow"], mesh.shape["pcol"]
    n_x, n_z, n_pieces, early = n_prow // 2, n_pcol // 2, 5, (1, 3)

    def local(slab, panel, pivots, inv_lower, inv_upper):
        (row_count, columns), (rows, nb) = slab.shape, panel.shape
        half = columns // 2
        pair = rows * 5 // 8
        hbm = pl.BlockSpec(memory_space=pltpu.HBM)
        dma = pltpu.SemaphoreType.DMA
        flops = 2 * row_count * nb * (nb + columns)
        return pl.pallas_call(
            functools.partial(kernel, n_x, n_z, early),
            out_shape=pltpu.VMEM(slab.shape, slab.dtype),
            in_specs=[
                hbm,
                hbm,
                hbm,
                hbm,
                hbm,
                hbm,
            ],
            out_specs=pl.BlockSpec(memory_space=pltpu.VMEM),
            scratch_shapes=[
                pltpu.VMEM((n_z, rows, nb), F32),
                pltpu.VMEM((rows, nb), F32),
                pltpu.VMEM((2, n_z, rows, nb), BF16),
                pltpu.VMEM((n_z, rows, columns), F32),
                pltpu.VMEM((n_z, rows, columns), F32),
                pltpu.VMEM((nb, nb), F32),
                pltpu.VMEM((nb, nb), F32),
                pltpu.VMEM((2, nb, nb), BF16),
                pltpu.VMEM((2, nb, half), F32),
                pltpu.VMEM((nb, half), F32),
                pltpu.VMEM((nb, half), F32),
                pltpu.VMEM((max(n_x - 1, 1), nb, half), F32),
                pltpu.VMEM((nb, half), F32),
                pltpu.VMEM((4, nb, half), F32),
                pltpu.VMEM((2, nb, 2 * columns), BF16),
                pltpu.SMEM((nb,), jnp.int32),
                pltpu.VMEM((1, nb), jnp.int32),
                pltpu.VMEM((2, 2, nb, half), F32),
                pltpu.VMEM((2, nb, columns), BF16),
                pltpu.VMEM((2, pair, columns), F32),
                pltpu.VMEM((pair, columns), F32),
                dma((6,)),
                dma((2 * (n_z - 1),)),
                dma((n_pieces * (n_z - 1),)),
                dma((n_z - 1,)),
                dma((2 * (n_z - 1),)),
                dma,
                dma,
                dma((max(n_x - 1, 1),)),
                dma((max(n_x - 1, 1),)),
                dma((3,)),
                dma((3,)),
                dma,
                dma((5,)),
                pltpu.VMEM((max(rows // 16, 8), columns), F32),
                pltpu.VMEM((2, rows // 8, columns), F32),
                dma((1 if n_z > 3 else 2,)),
                dma((1 if n_z > 3 else 2,)),
                dma,
                dma((1 if n_z > 3 else 2,)),
                dma((1 if n_z > 3 else 2,)),
                dma((1 if n_z > 3 else 2,)),
                dma,
                dma,
                dma,
            ],
            compiler_params=pltpu.CompilerParams(
                collective_id=0, has_side_effects=True, vmem_limit_bytes=32 * 2**20
            ),
            cost_estimate=pl.CostEstimate(
                flops=flops, bytes_accessed=8 * slab.size, transcendentals=0
            ),
        )(
            *(
                pltpu.with_memory_space_constraint(a, pltpu.HBM)
                for a in (slab, panel, pivots, pivots.reshape(1, nb), inv_lower, inv_upper)
            )
        )

    return jax.shard_map(
        local,
        mesh=mesh,
        in_specs=(P("prow", "pcol"), P(("prow", "pcol"), None), P(), P(), P()),
        out_specs=P("prow", "pcol"),
        check_vma=False,
    )
```
